32 devices in a mesh: dp: 8 (over z, x), mp: 4 (over y, core).
Axes of the slice: x: 2, y: 2, z: 4, core: 2. Of those that a mesh axis runs over, the one named last changes fastest.
Arguments:
- vlm_tokens: bfloat16 [2048, 2048], P(('dp', 'mp')), may hold values from -64 to 64
- action_tokens: bfloat16 [4096, 2048], P(('dp', 'mp')), may hold values from -64 to 64
- norm_gain: float32 [2048], replicated, may hold values from 0.25 to 1.75
- proj_old: bfloat16 [4096, 4096], P('dp', 'mp'), may hold values from -0.125 to 0.125
Outputs:
- vlm_hidden: bfloat16 [4096, 4096], P('dp', 'mp')
- action_hidden: bfloat16 [4096, 8192], P('dp', 'mp')
- proj_new: bfloat16 [2048, 8192], P('dp', 'mp')
The draws below stay inside these ranges and needn't reach their ends.
All inputs are finite; a program needn't handle non-finite values.
Results may differ from the reference program's by a relative error of at most 0.005.
Values may be sent and summed in bfloat16 or wider, within the bound.
A program may use at most 64 MiB of HBM per device.

```python
import math
import jax
import jax.numpy as jnp
from jax import lax

D = 2048
FF = 8192
VLM_TOK = 512
ACT_TOK = 512
VLM_ALL = 2048
ACT_ALL = 4096
N_DP = 8
N_MP = 4


def make_tokens(key, number_rows):
    key_base, key_column, key_row = jax.random.split(key, 3)
    entries = jax.random.normal(key_base, (number_rows, D), jnp.float32)
    column = jnp.exp(jax.random.uniform(key_column, (1, D), jnp.float32, math.log(0.3), math.log(3.0)))
    row_scale = jnp.exp(jax.random.uniform(key_row, (number_rows, 1), jnp.float32, 0.0, math.log(10.0)))
    return jnp.clip(entries * column * row_scale, -64.0, 64.0).astype(jnp.bfloat16)


def draw_vlm_tokens(key, part):
    return make_tokens(jax.random.fold_in(key, 11), VLM_ALL)


def draw_action_tokens(key, part):
    return make_tokens(jax.random.fold_in(key, 23), ACT_ALL)


def levels(key, dims, shards, low, top_value):
    level, own = 1.0, jax.random.fold_in(key, 6)
    for dim, parts in shards:
        heights = jnp.exp(jax.random.uniform(jax.random.fold_in(own, dim), (parts,), jnp.float32, low / len(shards), top_value / len(shards)))
        level = level * jnp.repeat(heights, dims[dim] // parts).reshape([-1 if axis == dim else 1 for axis in range(len(dims))])
    return level


def gaussian(key, dims, width, most, cuts=(), kind=jnp.bfloat16):
    factor_of = levels(key, dims, cuts, -0.22, 0.18) if cuts else 1.0
    values = jax.random.normal(key, dims, jnp.float32) * width * factor_of
    return jnp.minimum(jnp.maximum(values, -most), most).astype(kind)


def setup_inputs(seed: int = 0) -> dict:
    key_list = jax.random.split(jax.random.key(seed), 5)
    vlm_tokens = draw_vlm_tokens(jax.random.fold_in(key_list[4], 71), 0)
    action_tokens = draw_action_tokens(jax.random.fold_in(key_list[4], 71), 0)
    norm_gain = jnp.clip(1.0 + 0.15 * jax.random.normal(key_list[2], (D,), jnp.float32), 0.25, 1.75)
    proj_old = gaussian(key_list[3], (2 * D, FF // 2), D ** -0.5, 0.125, ((0, 8), (1, 4)))
    return dict(vlm_tokens=vlm_tokens, action_tokens=action_tokens, norm_gain=norm_gain, proj_old=proj_old)


epsilon = 1e-06

def normalize(row_values, norm_gain):
    values = row_values.astype(jnp.float32)
    factor = lax.rsqrt(lax.optimization_barrier(jnp.mean(values * values, axis=-1, keepdims=True)) + epsilon)
    return (values * factor * norm_gain).astype(jnp.bfloat16)

def reference(vlm_tokens, action_tokens, norm_gain, proj_old):
    groups = N_DP // 2
    row_block = 2 * D // N_DP
    col_block = FF // (2 * N_MP)
    weight = proj_old.reshape(groups, 2, row_block, N_MP, col_block).transpose(0, 2, 3, 1, 4).reshape(D, FF)

    def forward(tokens_block):
        normed = normalize(tokens_block, norm_gain)
        product = jnp.dot(normed, weight, preferred_element_type=jnp.float32)
        return jax.nn.gelu(product, approximate=False).astype(jnp.bfloat16)
    hidden_vlm = lax.map(forward, vlm_tokens.reshape(groups, VLM_TOK, D))
    vlm_hidden = hidden_vlm.reshape(groups, VLM_TOK, N_MP, 2, col_block).transpose(0, 3, 1, 2, 4).reshape(2 * VLM_ALL, FF // 2)
    action_hidden = lax.map(forward, action_tokens.reshape(N_DP, ACT_TOK, D)).reshape(ACT_ALL, FF)
    return (vlm_hidden, action_hidden, weight)
```

```python
import functools
import math
import jax
import jax.numpy as jnp
from jax import lax
from jax.experimental import pallas as pl
from jax.experimental.pallas import tpu as pltpu
from jax.sharding import PartitionSpec as P

MESH = pl.DeviceIdType.MESH
epsilon = 1e-06


def normalize(row_values, norm_gain):
    values = row_values.astype(jnp.float32)
    factor = lax.rsqrt(jnp.mean(values * values, axis=-1, keepdims=True) + epsilon)
    return (values * factor * norm_gain).astype(jnp.bfloat16)


def gelu(u):
    return (u * 0.5 * (1.0 + lax.erf(u * math.sqrt(0.5)))).astype(jnp.bfloat16)


def chunk_width(cols):
    return max(cols // 8, 128)


def kernel(groups, mp_size, vlm_hbm, act_hbm, gain_hbm, proj_hbm, vlm_out, act_out, new_out,
           vlm_ref, act_ref, gain_ref, tok, wbuf, hid, tok_send, tok_recv, w_send, w_recv, ex_send, ex_recv,
           hid_send, hid_recv, load_sem, loc_sem):
    d = lax.axis_index("dp")
    m = lax.axis_index("mp")
    g, p = d // 2, d % 2
    y, c = m // 2, m % 2
    vr, ar = vlm_ref.shape[0], act_ref.shape[0]
    r, cols = proj_hbm.shape
    half = r // 2
    width = chunk_width(cols)
    n = cols // width
    vlm_rows, act_rows = 2 * mp_size * vr, mp_size * ar
    sibling = (d, y * 2 + 1 - c)
    xpart = (g * 2 + 1 - p, m)
    ypart = (d, (1 - y) * 2 + c)
    has_left, has_right = g > 0, g < groups - 1

    def chunk(k, count=1):
        return pl.ds(pl.multiple_of(k * width, width), count * width)

    def block_rows(block):
        return pl.ds(pl.multiple_of(block * r, r), r)

    barrier = pltpu.get_barrier_semaphore()

    @pl.when(has_left)
    def _():
        pl.semaphore_signal(barrier, inc=1, device_id=(d - 2, m), device_id_type=MESH)

    @pl.when(has_right)
    def _():
        pl.semaphore_signal(barrier, inc=1, device_id=(d + 2, m), device_id_type=MESH)

    for other in (xpart, ypart, sibling):
        pl.semaphore_signal(barrier, inc=1, device_id=other, device_id_type=MESH)

    first_load = pltpu.make_async_copy(proj_hbm.at[:, chunk(0)], wbuf.at[block_rows(g), chunk(0)], load_sem.at[3])
    rest_load = pltpu.make_async_copy(
        proj_hbm.at[:, chunk(1, n - 1)], wbuf.at[block_rows(g), chunk(1, n - 1)], load_sem.at[4])
    loads = [pltpu.make_async_copy(src, dst, load_sem.at[i]) for i, (src, dst) in enumerate(
        ((gain_hbm, gain_ref), (vlm_hbm, vlm_ref), (act_hbm, act_ref)))]
    first_load.start()
    rest_load.start()
    for load in loads:
        load.start()
    pl.semaphore_wait(barrier, 3 + has_left.astype(jnp.int32) + has_right.astype(jnp.int32))

    def w_copy(block, cc, recv, side):
        return pltpu.make_async_remote_copy(
            src_ref=wbuf.at[block_rows(block), cc],
            dst_ref=wbuf.at[block_rows(block), cc],
            send_sem=w_send.at[side, block],
            recv_sem=recv,
            device_id=(d - 2 if side == 0 else d + 2, m),
            device_id_type=MESH,
        )

    def w_chunk(block, k, side):
        return w_copy(block, chunk(k), w_recv.at[block, k], side)

    def send_own(k):
        @pl.when(has_left)
        def _():
            w_chunk(g, k, 0).start()

        @pl.when(has_right)
        def _():
            w_chunk(g, k, 1).start()

    first_load.wait()
    send_own(0)
    rest_load.wait()
    send_own(1)
    for load in loads:
        load.wait()

    def token_rows(pp, mm):
        s = pp * mp_size + mm
        return (pl.ds(pl.multiple_of(s * vr, vr), vr), pl.ds(pl.multiple_of(vlm_rows + s * ar, ar), ar))

    step = 32

    @pl.loop(0, vr // step)
    def _(i):
        o = pl.multiple_of(i * step, step)
        tok[pl.ds(pl.multiple_of((p * mp_size + m) * vr + o, step), step), :] = normalize(
            vlm_ref[pl.ds(o, step), :], gain_ref[...])

    @pl.loop(0, ar // step)
    def _(i):
        o = pl.multiple_of(i * step, step)
        tok[pl.ds(pl.multiple_of(vlm_rows + (p * mp_size + m) * ar + o, step), step), :] = normalize(
            act_ref[pl.ds(o, step), :], gain_ref[...])

    def tok_copy(pp, mm, part, to, slot):
        rows = token_rows(pp, mm)[part]
        return pltpu.make_async_remote_copy(
            src_ref=tok.at[rows, :], dst_ref=tok.at[rows, :], send_sem=tok_send,
            recv_sem=tok_recv.at[slot, 0 if slot == 3 else part], device_id=to, device_id_type=MESH)

    m_y = (1 - y) * 2 + c
    for part in (1, 0):
        tok_copy(p, m, part, xpart, 0).start()
        tok_copy(p, m, part, ypart, 1).start()
    for part in (1, 0):
        tok_copy(p, m, part, sibling, 3).start()

    def relay_first():
        tok_copy(1 - p, m, 1, sibling, 0).wait_recv()
        tok_copy(1 - p, m, 1, ypart, 2).start()
        tok_copy(p, m_y, 1, sibling, 1).wait_recv()
        tok_copy(p, m_y, 0, sibling, 1).wait_recv()
        tok_copy(p, m_y, 0, xpart, 2).start()
        tok_copy(1 - p, m, 0, sibling, 0).wait_recv()
        for part in (1, 0):
            tok_copy(1 - p, m, part, sibling, 3).start()
            tok_copy(p, m_y, part, sibling, 3).start()

    def relay_second():
        for part in (0, 1):
            tok_copy(1 - p, m_y, part, sibling, 2).wait_recv()
            tok_copy(1 - p, m_y, part, sibling, 3).start()

    def all_tokens():
        count = mp_size * (vr + ar)
        there = tok.at[pl.ds(0, count), :]
        pltpu.make_async_remote_copy(
            src_ref=there, dst_ref=there, send_sem=tok_send, recv_sem=tok_recv.at[3, 0],
            device_id=sibling, device_id_type=MESH).wait_recv()

    ex = pltpu.make_async_remote_copy(
        src_ref=wbuf.at[pl.ds(pl.multiple_of(g * r + (1 - p) * half, half), half), :],
        dst_ref=new_out.at[:, pl.ds(pl.multiple_of(p * cols, cols), cols)],
        send_sem=ex_send, recv_sem=ex_recv, device_id=xpart, device_id_type=MESH)
    kept = pltpu.make_async_copy(
        wbuf.at[pl.ds(pl.multiple_of(g * r + p * half, half), half), :],
        new_out.at[:, pl.ds(pl.multiple_of(p * cols, cols), cols)], loc_sem.at[0])

    def arrive(t):
        own = t + 2 if isinstance(t, int) else t + 2

        @pl.when(own < n)
        def _():
            send_own(own)

        @pl.loop(0, groups - 1)
        def _(i):
            k = t - i

            @pl.when((k >= 0) & (k < n) & (g - 1 - i >= 0))
            def _():
                w_chunk(g - 1 - i, k, 1).wait_recv()

                @pl.when(has_right)
                def _():
                    w_chunk(g - 1 - i, k, 1).start()

            @pl.when((k >= 0) & (k < n) & (g + 1 + i < groups))
            def _():
                w_chunk(g + 1 + i, k, 0).wait_recv()

                @pl.when(has_left)
                def _():
                    w_chunk(g + 1 + i, k, 0).start()

    tile = math.gcd(256, math.gcd(vlm_rows, act_rows))
    a_tiles, v_tiles = act_rows // tile, vlm_rows // tile

    def out_cols(side, cc):
        return pl.ds(pl.multiple_of(side * cols + cc.start, cc.size), cc.size)

    def tile_rows(start):
        return pl.ds(pl.multiple_of(start, tile), tile)

    def hid_copy(cc, t):
        return pltpu.make_async_remote_copy(
            src_ref=hid.at[tile_rows(vlm_rows + (1 - p) * act_rows + t * tile), cc],
            dst_ref=act_out.at[tile_rows(t * tile), out_cols(p, cc)],
            send_sem=hid_send, recv_sem=hid_recv, device_id=xpart, device_id_type=MESH)

    def own_copy(cc):
        return pltpu.make_async_copy(
            hid.at[pl.ds(pl.multiple_of(vlm_rows + p * act_rows, act_rows), act_rows), cc],
            act_out.at[:, out_cols(p, cc)], loc_sem.at[1])

    def vlm_copy(cc):
        return pltpu.make_async_copy(hid.at[pl.ds(0, vlm_rows), cc], vlm_out.at[:, cc], loc_sem.at[2])

    def hidden(rows, cc):
        pre = jnp.dot(tok[rows, :], wbuf[:, cc], preferred_element_type=jnp.float32)
        hid[rows, cc] = gelu(pre)

    def for_partner(cc):
        @pl.loop(0, a_tiles)
        def _(t):
            hidden(tile_rows(vlm_rows + (1 - p) * act_rows + t * tile), cc)
            hid_copy(cc, t).start()

    def for_self(cc):
        @pl.loop(0, a_tiles + v_tiles)
        def _(t):
            hidden(tile_rows(jnp.where(
                t < a_tiles, vlm_rows + p * act_rows + t * tile, (t - a_tiles) * tile)), cc)

    warm = groups - 1

    @pl.loop(0, warm)
    def _(t):
        arrive(t)

    relay_first()
    ex.start()
    kept.start()
    arrive(warm)
    arrive(warm + 1)
    relay_second()
    all_tokens()
    for j in range(0, n - 2, 2):
        if j:
            for t in (warm + j - 1, warm + j):
                if t > warm + 1:
                    arrive(t)
        for_partner(chunk(j, 2))
        for_self(chunk(j, 2))
    for j in (n - 2, n - 1):
        arrive(warm + j - 1)
        for_partner(chunk(j))
    for_self(chunk(n - 2, 2))
    own_copy(pl.ds(0, cols)).start()
    vlm_copy(pl.ds(0, cols)).start()

    count = 7 * (vr + ar)
    sent = tok.at[pl.ds(0, count), :]
    pltpu.make_async_remote_copy(
        src_ref=sent, dst_ref=sent, send_sem=tok_send, recv_sem=tok_recv.at[3, 0],
        device_id=sibling, device_id_type=MESH).wait_send()

    @pl.loop(0, groups)
    def _(block):
        @pl.when(has_left & (block >= g))
        def _():
            w_copy(block, pl.ds(0, cols), w_recv.at[block, 0], 0).wait_send()

        @pl.when(has_right & (block <= g))
        def _():
            w_copy(block, pl.ds(0, cols), w_recv.at[block, 0], 1).wait_send()

    ex.wait_send()
    taken = new_out.at[:, pl.ds(pl.multiple_of((1 - p) * cols, cols), cols)]
    pltpu.make_async_remote_copy(
        src_ref=taken, dst_ref=taken, send_sem=ex_send, recv_sem=ex_recv,
        device_id=xpart, device_id_type=MESH).wait_recv()
    kept.wait()
    own_copy(pl.ds(0, cols)).wait()
    vlm_copy(pl.ds(0, cols)).wait()
    there = act_out.at[:, pl.ds(pl.multiple_of((1 - p) * cols, cols), cols)]
    back = pltpu.make_async_remote_copy(
        src_ref=there, dst_ref=there, send_sem=hid_send, recv_sem=hid_recv,
        device_id=xpart, device_id_type=MESH)
    back.wait_send()
    back.wait_recv()


def store(*refs):
    count = (len(refs) - 1) // 2
    copies = [pltpu.make_async_copy(refs[i], refs[count + i], refs[-1].at[i]) for i in range(count)]
    for copy in copies:
        copy.start()
    for copy in copies:
        copy.wait()


def solution(mesh):
    groups, mp_size = mesh.shape["dp"] // 2, mesh.shape["mp"]

    def local(vlm_tokens, action_tokens, norm_gain, proj_old):
        vr, ar = vlm_tokens.shape[0], action_tokens.shape[0]
        features = vlm_tokens.shape[1]
        r, cols = proj_old.shape
        vlm_rows, act_rows = 2 * mp_size * vr, mp_size * ar
        bf16 = jnp.bfloat16
        dma = pltpu.SemaphoreType.DMA
        hbm, anywhere = pl.BlockSpec(memory_space=pltpu.HBM), pl.BlockSpec(memory_space=pl.ANY)
        chunks = cols // chunk_width(cols)
        shapes = (
            jax.ShapeDtypeStruct((vlm_rows, cols), bf16),
            jax.ShapeDtypeStruct((act_rows, 2 * cols), bf16),
            jax.ShapeDtypeStruct((r // 2, 2 * cols), bf16),
        )
        results = pl.pallas_call(
            functools.partial(kernel, groups, mp_size),
            name="up_gelu",
            out_shape=shapes,
            in_specs=[hbm] * 4,
            out_specs=(anywhere,) * 3,
            scratch_shapes=[
                pltpu.VMEM((vr, features), bf16),
                pltpu.VMEM((ar, features), bf16),
                pltpu.VMEM((1, features), jnp.float32),
                pltpu.VMEM((vlm_rows + 2 * act_rows, features), bf16),
                pltpu.VMEM((groups * r, cols), bf16),
                pltpu.VMEM((vlm_rows + 2 * act_rows, cols), bf16),
                dma, dma((4, 2)), dma((2, groups)), dma((groups, chunks)), dma, dma, dma, dma, dma((5,)), dma((3,)),
            ],
            compiler_params=pltpu.CompilerParams(
                collective_id=0, has_side_effects=True, vmem_limit_bytes=48 * 1024 * 1024),
        )(*[pltpu.with_memory_space_constraint(array, pltpu.HBM) for array in (
            vlm_tokens, action_tokens, norm_gain.reshape(1, -1), proj_old)])
        return pl.pallas_call(
            store,
            name="store",
            out_shape=shapes,
            in_specs=[anywhere] * 3,
            out_specs=(hbm,) * 3,
            scratch_shapes=[dma((3,))],
            compiler_params=pltpu.CompilerParams(vmem_limit_bytes=1024 * 1024),
        )(*results)

    return jax.shard_map(
        local,
        mesh=mesh,
        in_specs=(P(("dp", "mp"), None), P(("dp", "mp"), None), P(), P("dp", "mp")),
        out_specs=(P("dp", "mp"), P("dp", "mp"), P("dp", "mp")),
        check_vma=False,
    )
```

```python
import functools
import math
import jax
import jax.numpy as jnp
from jax import lax
from jax.experimental import pallas as pl
from jax.experimental.pallas import tpu as pltpu
from jax.sharding import PartitionSpec as P

MESH = pl.DeviceIdType.MESH
epsilon = 1e-06


def normalize(row_values, norm_gain):
    values = row_values.astype(jnp.float32)
    factor = lax.rsqrt(jnp.mean(values * values, axis=-1, keepdims=True) + epsilon)
    return (values * factor * norm_gain).astype(jnp.bfloat16)


def gelu(u):
    return (u * 0.5 * (1.0 + lax.erf(u * math.sqrt(0.5)))).astype(jnp.bfloat16)


def chunk_width(cols):
    return max(cols // 8, 128)


def kernel(groups, mp_size, vlm_hbm, act_hbm, gain_hbm, proj_hbm, vlm_out, act_out, new_out,
           vlm_ref, act_ref, gain_ref, tok, wbuf, hid, tok_send, tok_recv, w_send, w_recv, ex_send, ex_recv,
           hid_send, hid_recv, load_sem, loc_sem, far_tok, far_w, far_hid, ft_send, ft_recv, fw_send, fw_recv,
           fh_send, fh_recv):
    d = lax.axis_index("dp")
    m = lax.axis_index("mp")
    g, p = d // 2, d % 2
    y, c = m // 2, m % 2
    vr, ar = vlm_ref.shape[0], act_ref.shape[0]
    r, cols = proj_hbm.shape
    half = r // 2
    width = chunk_width(cols)
    n = cols // width
    vlm_rows, act_rows = 2 * mp_size * vr, mp_size * ar
    sibling = (d, y * 2 + 1 - c)
    xpart = (g * 2 + 1 - p, m)
    ypart = (d, (1 - y) * 2 + c)
    has_left, has_right = g > 0, g < groups - 1
    far = groups >= 4 and n >= 8
    end = (g == 0) | (g == groups - 1)
    near = ((g == 1) | (g == groups - 2)) & far
    short = end & (c == 0) & far
    toward = jnp.where(g <= 1, 0, groups - 1)
    inward = jnp.where(g == 0, 1, groups - 2)

    def chunk(k, count=1):
        return pl.ds(pl.multiple_of(k * width, width), count * width)

    def block_rows(block):
        return pl.ds(pl.multiple_of(block * r, r), r)

    barrier = pltpu.get_barrier_semaphore()

    @pl.when(has_left)
    def _():
        pl.semaphore_signal(barrier, inc=1, device_id=(d - 2, m), device_id_type=MESH)

    @pl.when(has_right)
    def _():
        pl.semaphore_signal(barrier, inc=1, device_id=(d + 2, m), device_id_type=MESH)

    for other in (xpart, ypart, sibling):
        pl.semaphore_signal(barrier, inc=1, device_id=other, device_id_type=MESH)

    first_load = pltpu.make_async_copy(proj_hbm.at[:, chunk(0)], wbuf.at[block_rows(g), chunk(0)], load_sem.at[3])
    rest_load = pltpu.make_async_copy(
        proj_hbm.at[:, chunk(1, n - 1)], wbuf.at[block_rows(g), chunk(1, n - 1)], load_sem.at[4])
    loads = [pltpu.make_async_copy(src, dst, load_sem.at[i]) for i, (src, dst) in enumerate(
        ((gain_hbm, gain_ref), (vlm_hbm, vlm_ref), (act_hbm, act_ref)))]
    first_load.start()
    rest_load.start()
    for load in loads:
        load.start()

    @pl.when(near & (c == 1))
    def _():
        pl.semaphore_signal(barrier, inc=1, device_id=(toward * 2 + p, y * 2), device_id_type=MESH)

    pl.semaphore_wait(barrier, 3 + sum(flag.astype(jnp.int32) for flag in (has_left, has_right, short)))

    def w_copy(block, cc, recv, side):
        return pltpu.make_async_remote_copy(
            src_ref=wbuf.at[block_rows(block), cc],
            dst_ref=wbuf.at[block_rows(block), cc],
            send_sem=w_send.at[jnp.where((block == g) & (side == 0), groups, block)],
            recv_sem=recv,
            device_id=(d - 2 if side == 0 else d + 2, m),
            device_id_type=MESH,
        )

    def w_chunk(block, k, side):
        return w_copy(block, chunk(k), w_recv.at[lax.rem(block - g + 2 * groups + (0 if side == 0 else -2), groups), k], side)

    def w_arrival(block, k):
        there = wbuf.at[block_rows(block), chunk(k)]
        return pltpu.make_async_remote_copy(
            src_ref=there, dst_ref=there, send_sem=w_send.at[block],
            recv_sem=w_recv.at[lax.rem(block - g + 2 * groups - 1, groups), k],
            device_id=sibling, device_id_type=MESH)

    short_left = near & (g == 1) & (c == 0)
    short_right = near & (g == groups - 2) & (c == 0)

    def send_w(block, k, side):
        ok, brief = (has_left, short_left) if side == 0 else (has_right, short_right)

        @pl.when(ok & jnp.logical_not(brief & (k == 0)))
        def _():
            w_chunk(block, k, side).start()

    def send_own(k):
        send_w(g, k, 0)
        send_w(g, k, 1)

    first_load.wait()
    send_own(0)
    rest_load.wait()
    send_own(1)

    @pl.when(end)
    def _():
        @pl.loop(2, n)
        def _(k):
            send_own(k)

    for load in loads:
        load.wait()

    def token_rows(pp, mm):
        s = pp * mp_size + mm
        return (pl.ds(pl.multiple_of(s * vr, vr), vr), pl.ds(pl.multiple_of(vlm_rows + s * ar, ar), ar))

    step = 32

    @pl.loop(0, vr // step)
    def _(i):
        o = pl.multiple_of(i * step, step)
        tok[pl.ds(pl.multiple_of((p * mp_size + m) * vr + o, step), step), :] = normalize(
            vlm_ref[pl.ds(o, step), :], gain_ref[...])

    @pl.loop(0, ar // step)
    def _(i):
        o = pl.multiple_of(i * step, step)
        tok[pl.ds(pl.multiple_of(vlm_rows + (p * mp_size + m) * ar + o, step), step), :] = normalize(
            act_ref[pl.ds(o, step), :], gain_ref[...])

    def tok_copy(pp, mm, part, to, slot):
        rows = token_rows(pp, mm)[part]
        return pltpu.make_async_remote_copy(
            src_ref=tok.at[rows, :], dst_ref=tok.at[rows, :], send_sem=tok_send,
            recv_sem=tok_recv.at[slot, 0 if slot == 3 else part], device_id=to, device_id_type=MESH)

    m_y = (1 - y) * 2 + c
    for part in (1, 0):
        tok_copy(p, m, part, xpart, 0).start()
        tok_copy(p, m, part, ypart, 1).start()
    for part in (1, 0):
        tok_copy(p, m, part, sibling, 3).start()

    def far_token_copy(part, c_from):
        rows = token_rows(p, m)[part]
        at = pl.ds(pl.multiple_of(c_from * (vr + ar) + part * vr, math.gcd(vr, ar)), (vr, ar)[part])
        return pltpu.make_async_remote_copy(
            src_ref=tok.at[rows, :], dst_ref=far_tok.at[at, :], send_sem=ft_send, recv_sem=ft_recv,
            device_id=(inward * 2 + p, y * 2 + 1), device_id_type=MESH)

    if far:
        @pl.when(end)
        def _():
            for part in (0, 1):
                far_token_copy(part, c).start()

    def far_w_copy(panel, to, slot):
        at = far_w.at[:, pl.ds(pl.multiple_of(panel * width, width), width)]
        return pltpu.make_async_remote_copy(
            src_ref=at if slot == 3 else wbuf.at[:, chunk(0)], dst_ref=at, send_sem=fw_send, recv_sem=fw_recv.at[slot],
            device_id=to, device_id_type=MESH)

    def spread_far_w():
        @pl.when(near & (c == 0))
        def _():
            far_w_copy(y * 2 + p, (g * 2 + 1 - p, y * 2 + 1), 1).start()
            far_w_copy(y * 2 + p, (d, (1 - y) * 2 + 1), 2).start()
            far_w_copy(y * 2 + p, sibling, 0).start()

    def relay_far_w():
        @pl.when(near & (c == 1))
        def _():
            far_w_copy(y * 2 + 1 - p, ypart, 1).wait_recv()
            far_w_copy(y * 2 + 1 - p, ypart, 3).start()

    def far_hid_copies(same_chip):
        for c_from in (0, 1):
            base = c_from * (vr + ar)
            m_from = y * 2 + c_from
            for step_y in (0, 1):
                y_to = y if step_y == 0 else 1 - y
                for step_p in (0, 1):
                    b = p if step_p == 0 else 1 - p
                    cols_at = pl.ds(pl.multiple_of((y_to * 2 + b) * width, width), width)
                    if (step_y == 0 and step_p == 0) == same_chip:
                        yield pltpu.make_async_remote_copy(
                            src_ref=far_hid.at[pl.ds(base, vr), cols_at],
                            dst_ref=vlm_out.at[pl.ds(pl.multiple_of((p * mp_size + m_from) * vr, vr), vr), chunk(0)],
                            send_sem=fh_send, recv_sem=fh_recv, device_id=(toward * 2 + b, y_to * 2), device_id_type=MESH)
                    if (step_y == 0) == same_chip:
                        yield pltpu.make_async_remote_copy(
                            src_ref=far_hid.at[pl.ds(base + vr, ar), cols_at],
                            dst_ref=act_out.at[pl.ds(pl.multiple_of(m_from * ar, ar), ar), out_cols(b, chunk(0))],
                            send_sem=fh_send, recv_sem=fh_recv, device_id=(toward * 2 + p, y_to * 2), device_id_type=MESH)

    def far_compute():
        @pl.when(near & (c == 1))
        def _():
            pltpu.make_async_remote_copy(
                src_ref=far_tok, dst_ref=far_tok, send_sem=ft_send, recv_sem=ft_recv,
                device_id=sibling, device_id_type=MESH).wait_recv()
            far_w_copy(y * 2, sibling, 0).wait_recv()
            far_w_copy(y * 2, sibling, 2).wait_recv()
            far_w_copy(y * 2, sibling, 3).wait_recv()

            @pl.loop(0, 2)
            def _(i):
                rows = pl.ds(pl.multiple_of(i * (vr + ar), math.gcd(vr, ar)), vr + ar)

                @pl.loop(0, 2)
                def _(j):
                    at = pl.ds(pl.multiple_of(j * 2 * width, width), 2 * width)
                    pre = jnp.dot(far_tok[rows, :], far_w[:, at], preferred_element_type=jnp.float32)
                    far_hid[rows, at] = gelu(pre)

            for copy in far_hid_copies(True):
                copy.start()

    def relay_first():
        tok_copy(1 - p, m, 1, sibling, 0).wait_recv()
        tok_copy(1 - p, m, 1, ypart, 2).start()
        tok_copy(p, m_y, 1, sibling, 1).wait_recv()
        tok_copy(p, m_y, 0, sibling, 1).wait_recv()
        tok_copy(p, m_y, 0, xpart, 2).start()
        tok_copy(1 - p, m, 0, sibling, 0).wait_recv()
        for part in (1, 0):
            tok_copy(1 - p, m, part, sibling, 3).start()
            tok_copy(p, m_y, part, sibling, 3).start()

    def relay_second():
        for part in (0, 1):
            tok_copy(1 - p, m_y, part, sibling, 2).wait_recv()
            tok_copy(1 - p, m_y, part, sibling, 3).start()

    def all_tokens():
        count = mp_size * (vr + ar)
        there = tok.at[pl.ds(0, count), :]
        pltpu.make_async_remote_copy(
            src_ref=there, dst_ref=there, send_sem=tok_send, recv_sem=tok_recv.at[3, 0],
            device_id=sibling, device_id_type=MESH).wait_recv()

    ex = pltpu.make_async_remote_copy(
        src_ref=wbuf.at[pl.ds(pl.multiple_of(g * r + (1 - p) * half, half), half), :],
        dst_ref=new_out.at[:, pl.ds(pl.multiple_of(p * cols, cols), cols)],
        send_sem=ex_send, recv_sem=ex_recv, device_id=xpart, device_id_type=MESH)
    kept = pltpu.make_async_copy(
        wbuf.at[pl.ds(pl.multiple_of(g * r + p * half, half), half), :],
        new_out.at[:, pl.ds(pl.multiple_of(p * cols, cols), cols)], loc_sem.at[0])

    def arrive(t):
        @pl.when((t + 2 < n) & jnp.logical_not(end))
        def _():
            send_own(t + 2)

        @pl.loop(0, groups - 1)
        def _(i):
            k = t - i

            inside = (k >= 0) & (k < n) & jnp.logical_not(short & (k == 0))

            @pl.when(inside & (g - 1 - i >= 0))
            def _():
                w_arrival(g - 1 - i, k).wait_recv()
                send_w(g - 1 - i, k, 1)

            @pl.when(inside & (g + 1 + i < groups))
            def _():
                w_arrival(g + 1 + i, k).wait_recv()
                send_w(g + 1 + i, k, 0)

    tile = math.gcd(256, math.gcd(vlm_rows, act_rows))
    a_tiles, v_tiles = act_rows // tile, vlm_rows // tile

    def out_cols(side, cc):
        return pl.ds(pl.multiple_of(side * cols + cc.start, width), cc.size)

    def tile_rows(start):
        return pl.ds(pl.multiple_of(start, tile), tile)

    def hid_copy(cc, t):
        return pltpu.make_async_remote_copy(
            src_ref=hid.at[tile_rows(vlm_rows + (1 - p) * act_rows + t * tile), cc],
            dst_ref=act_out.at[tile_rows(t * tile), out_cols(p, cc)],
            send_sem=hid_send, recv_sem=hid_recv, device_id=xpart, device_id_type=MESH)

    def own_copy(cc):
        return pltpu.make_async_copy(
            hid.at[pl.ds(pl.multiple_of(vlm_rows + p * act_rows, act_rows), act_rows), cc],
            act_out.at[:, out_cols(p, cc)], loc_sem.at[1])

    def vlm_copy(cc):
        return pltpu.make_async_copy(hid.at[pl.ds(0, vlm_rows), cc], vlm_out.at[:, cc], loc_sem.at[2])

    def hidden(rows, cc):
        pre = jnp.dot(tok[rows, :], wbuf[:, cc], preferred_element_type=jnp.float32)
        hid[rows, cc] = gelu(pre)

    def for_partner(cc):
        @pl.loop(0, a_tiles)
        def _(t):
            hidden(tile_rows(vlm_rows + (1 - p) * act_rows + t * tile), cc)
            hid_copy(cc, t).start()

    def for_self(cc):
        @pl.loop(0, a_tiles + v_tiles)
        def _(t):
            hidden(tile_rows(jnp.where(
                t < a_tiles, vlm_rows + p * act_rows + t * tile, (t - a_tiles) * tile)), cc)

    warm = groups - 1

    @pl.loop(0, warm)
    def _(t):
        arrive(t)

    relay_first()
    if far:
        spread_far_w()
    ex.start()
    kept.start()
    arrive(warm)
    arrive(warm + 1)
    relay_second()
    if far:
        relay_far_w()
    all_tokens()

    def first_pair():
        if far:
            @pl.when(short)
            def _():
                for_partner(chunk(1))
                for_self(chunk(1))

            @pl.when(jnp.logical_not(short))
            def _():
                for_partner(chunk(0, 2))
                for_self(chunk(0, 2))
        else:
            for_partner(chunk(0, 2))
            for_self(chunk(0, 2))

    first_pair()
    for j in range(2, n - 2, 2):
        for t in (warm + j - 1, warm + j):
            if t > warm + 1:
                arrive(t)
        for_partner(chunk(j, 2))
        for_self(chunk(j, 2))
    arrive(warm + n - 3)
    for_partner(chunk(n - 2))
    arrive(warm + n - 2)
    if far:
        far_compute()
    for_partner(chunk(n - 1))
    for_self(chunk(n - 2, 2))

    tail_cols, all_cols = chunk(1, n - 1), chunk(0, n)

    def by_width(brief, body):
        @pl.when(brief)
        def _():
            body(tail_cols)

        @pl.when(jnp.logical_not(brief))
        def _():
            body(all_cols)

    def copy_out(cc):
        own_copy(cc).start()
        vlm_copy(cc).start()

    def copied_out(cc):
        own_copy(cc).wait()
        vlm_copy(cc).wait()

    by_width(short, copy_out)

    @pl.loop(0, groups)
    def _(block):
        @pl.when(has_left & (block >= g))
        def _():
            by_width(short_left, lambda cc: w_copy(block, cc, ex_recv, 0).wait_send())

        @pl.when(has_right & (block <= g))
        def _():
            by_width(short_right, lambda cc: w_copy(block, cc, ex_recv, 1).wait_send())

    def bytes_of(ref, send, recv):
        return pltpu.make_async_remote_copy(
            src_ref=ref, dst_ref=ref, send_sem=send, recv_sem=recv, device_id=sibling, device_id_type=MESH)

    if far:
        @pl.when(near & (c == 1))
        def _():
            for copy in far_hid_copies(False):
                copy.start()
            bytes_of(far_w.at[:, pl.ds(0, width)], fw_send, ex_recv).wait_send()
            bytes_of(hid.at[pl.ds(0, 8 * (vr + ar)), chunk(0)], fh_send, ex_recv).wait_send()

        @pl.when(near & (c == 0))
        def _():
            bytes_of(wbuf.at[:, pl.ds(0, 3 * width)], fw_send, ex_recv).wait_send()

        @pl.when(end)
        def _():
            bytes_of(tok.at[pl.ds(0, vr + ar), :], ft_send, ex_recv).wait_send()

    bytes_of(tok.at[pl.ds(0, 7 * (vr + ar)), :], tok_send, ex_recv).wait_send()
    ex.wait_send()
    taken = new_out.at[:, pl.ds(pl.multiple_of((1 - p) * cols, cols), cols)]
    bytes_of(taken, ex_send, ex_recv).wait_recv()
    kept.wait()

    def exchanged(cc):
        there = act_out.at[:, out_cols(1 - p, cc)]
        bytes_of(there, hid_send, hid_recv).wait_send()
        bytes_of(there, hid_send, hid_recv).wait_recv()

    by_width(short, copied_out)
    by_width(short, exchanged)
    if far:
        @pl.when(short)
        def _():
            bytes_of(hid.at[:, chunk(0)], fh_send, fh_recv).wait_recv()


def store(*refs):
    count = (len(refs) - 1) // 2
    copies = [pltpu.make_async_copy(refs[i], refs[count + i], refs[-1].at[i]) for i in range(count)]
    for copy in copies:
        copy.start()
    for copy in copies:
        copy.wait()


def solution(mesh):
    groups, mp_size = mesh.shape["dp"] // 2, mesh.shape["mp"]

    def local(vlm_tokens, action_tokens, norm_gain, proj_old):
        vr, ar = vlm_tokens.shape[0], action_tokens.shape[0]
        features = vlm_tokens.shape[1]
        r, cols = proj_old.shape
        vlm_rows, act_rows = 2 * mp_size * vr, mp_size * ar
        bf16 = jnp.bfloat16
        dma = pltpu.SemaphoreType.DMA
        hbm, anywhere = pl.BlockSpec(memory_space=pltpu.HBM), pl.BlockSpec(memory_space=pl.ANY)
        chunks = cols // chunk_width(cols)
        shapes = (
            jax.ShapeDtypeStruct((vlm_rows, cols), bf16),
            jax.ShapeDtypeStruct((act_rows, 2 * cols), bf16),
            jax.ShapeDtypeStruct((r // 2, 2 * cols), bf16),
        )
        results = pl.pallas_call(
            functools.partial(kernel, groups, mp_size),
            name="up_gelu",
            out_shape=shapes,
            in_specs=[hbm] * 4,
            out_specs=(anywhere,) * 3,
            scratch_shapes=[
                pltpu.VMEM((vr, features), bf16),
                pltpu.VMEM((ar, features), bf16),
                pltpu.VMEM((1, features), jnp.float32),
                pltpu.VMEM((vlm_rows + 2 * act_rows, features), bf16),
                pltpu.VMEM((groups * r, cols), bf16),
                pltpu.VMEM((vlm_rows + 2 * act_rows, cols), bf16),
                dma, dma((4, 2)), dma((groups + 1,)), dma((groups - 1, chunks)), dma, dma, dma, dma, dma((5,)), dma((3,)),
                pltpu.VMEM((2 * (vr + ar), features), bf16),
                pltpu.VMEM((groups * r, 4 * chunk_width(cols)), bf16),
                pltpu.VMEM((2 * (vr + ar), 4 * chunk_width(cols)), bf16),
                dma, dma, dma, dma((4,)), dma, dma,
            ],
            compiler_params=pltpu.CompilerParams(
                collective_id=0, has_side_effects=True, vmem_limit_bytes=48 * 1024 * 1024),
        )(*[pltpu.with_memory_space_constraint(array, pltpu.HBM) for array in (
            vlm_tokens, action_tokens, norm_gain.reshape(1, -1), proj_old)])
        return pl.pallas_call(
            store,
            name="store",
            out_shape=shapes,
            in_specs=[anywhere] * 3,
            out_specs=(hbm,) * 3,
            scratch_shapes=[dma((3,))],
            compiler_params=pltpu.CompilerParams(vmem_limit_bytes=1024 * 1024),
        )(*results)

    return jax.shard_map(
        local,
        mesh=mesh,
        in_specs=(P(("dp", "mp"), None), P(("dp", "mp"), None), P(), P("dp", "mp")),
        out_specs=(P("dp", "mp"), P("dp", "mp"), P("dp", "mp")),
        check_vma=False,
    )
```

```python
import functools
import math
import jax
import jax.numpy as jnp
from jax import lax
from jax.experimental import pallas as pl
from jax.experimental.pallas import tpu as pltpu
from jax.sharding import PartitionSpec as P

MESH = pl.DeviceIdType.MESH
epsilon = 1e-06


def normalize(row_values, norm_gain):
    values = row_values.astype(jnp.float32)
    factor = lax.rsqrt(jnp.mean(values * values, axis=-1, keepdims=True) + epsilon)
    return (values * factor * norm_gain).astype(jnp.bfloat16)


def gelu(u):
    return (u * 0.5 * (1.0 + lax.erf(u * math.sqrt(0.5)))).astype(jnp.bfloat16)


def chunk_width(cols):
    return max(cols // 8, 128)


def kernel(groups, mp_size, vlm_hbm, act_hbm, gain_hbm, proj_hbm, vlm_out, act_out, new_out,
           vlm_ref, act_ref, gain_ref, tok, wbuf, hid, tok_send, tok_recv, w_send, w_recv, ex_send, ex_recv,
           hid_send, hid_recv, load_sem, loc_sem, far_tok, far_w, far_hid, ft_send, ft_recv, fw_send, fw_recv,
           fh_send, fh_recv, ready):
    d = lax.axis_index("dp")
    m = lax.axis_index("mp")
    g, p = d // 2, d % 2
    y, c = m // 2, m % 2
    vr, ar = vlm_ref.shape[0], act_ref.shape[0]
    r, cols = proj_hbm.shape
    half = r // 2
    width = chunk_width(cols)
    n = cols // width
    vlm_rows, act_rows = 2 * mp_size * vr, mp_size * ar
    sibling = (d, y * 2 + 1 - c)
    xpart = (g * 2 + 1 - p, m)
    ypart = (d, (1 - y) * 2 + c)
    has_left, has_right = g > 0, g < groups - 1
    far = groups >= 4 and n >= 8
    late = 2
    end = (g == 0) | (g == groups - 1)
    near = ((g == 1) | (g == groups - 2)) & far
    short = end & (c == 0) & far
    toward = jnp.where(g <= 1, 0, groups - 1)
    inward = jnp.where(g == 0, 1, groups - 2)

    def chunk(k, count=1):
        return pl.ds(pl.multiple_of(k * width, width), count * width)

    def block_rows(block):
        return pl.ds(pl.multiple_of(block * r, r), r)

    barrier = pltpu.get_barrier_semaphore()

    left, right = (d - 2, m), (d + 2, m)
    earlier = ((has_left, left), (p == 1, xpart), (y == 1, ypart), (c == 1, sibling))
    later = ((has_right, right), (p == 0, xpart), (y == 0, ypart), (c == 0, sibling))

    def number(flags):
        return sum(flag.astype(jnp.int32) for flag in flags)

    def greet(semaphore, others):
        for flag, other in others:
            @pl.when(flag)
            def _():
                pl.semaphore_signal(semaphore, inc=1, device_id=other, device_id_type=MESH)

    greet(barrier, later + ((near & (c == 1), (toward * 2 + p, y * 2)),))
    w_load = pltpu.make_async_copy(proj_hbm, wbuf.at[block_rows(g), :], load_sem.at[3])
    loads = [pltpu.make_async_copy(src, dst, load_sem.at[i]) for i, (src, dst) in enumerate(
        ((gain_hbm, gain_ref), (vlm_hbm, vlm_ref), (act_hbm, act_ref)))]
    for load in loads:
        load.start()
    w_load.start()
    pl.semaphore_wait(barrier, number([flag for flag, _ in earlier] + [short]))
    greet(ready, earlier)

    brief = (near & (g == 1) & (c == 0), near & (g == groups - 2) & (c == 0))
    last = (near & (g == 1), near & (g == groups - 2))

    def w_copy(block, cc, send, recv, side, from_hbm=False):
        there = wbuf.at[block_rows(block), cc]
        return pltpu.make_async_remote_copy(
            src_ref=proj_hbm.at[:, cc] if from_hbm else there,
            dst_ref=there,
            send_sem=w_send.at[send],
            recv_sem=recv,
            device_id=left if side == 0 else right,
            device_id_type=MESH,
        )

    def w_slot(block, side):
        return jnp.where((block == g) & (side == 0), groups, block)

    def w_last(block, side):
        return last[side] & (block == (groups - 1 if side == 0 else 0))

    def w_chunk(block, k, side, from_hbm=False):
        return w_copy(
            block, chunk(k), jnp.where(w_last(block, side) & (k >= n - late), groups + 1, w_slot(block, side)),
            w_recv.at[lax.rem(block - g + 2 * groups + (0 if side == 0 else -2), groups), k], side, from_hbm)

    def w_arrival(block, k):
        there = wbuf.at[block_rows(block), chunk(k)]
        return pltpu.make_async_remote_copy(
            src_ref=there, dst_ref=there, send_sem=w_send.at[block],
            recv_sem=w_recv.at[lax.rem(block - g + 2 * groups - 1, groups), k],
            device_id=sibling, device_id_type=MESH)

    def send_w(block, k, side, from_hbm=False):
        ok = has_left if side == 0 else has_right

        @pl.when(ok & jnp.logical_not(brief[side] & (k == 0)))
        def _():
            w_chunk(block, k, side, from_hbm).start()

    def send_own(k):
        send_w(g, k, 0)
        send_w(g, k, 1)

    for k in (0, 1):
        send_w(g, k, 0, True)
    answers = number([flag for flag, _ in later])

    @pl.when(answers > 0)
    def _():
        pl.semaphore_wait(ready, answers)

    for k in (0, 1):
        send_w(g, k, 1, True)
    w_load.wait()
    for side in (0, 1):
        @pl.when(brief[side])
        def _():
            for k in (2, 3):
                send_w(g, k, side)


    @pl.when(end)
    def _():
        @pl.loop(2, n)
        def _(k):
            send_own(k)

    for load in loads:
        load.wait()

    def token_rows(pp, mm):
        s = pp * mp_size + mm
        return (pl.ds(pl.multiple_of(s * vr, vr), vr), pl.ds(pl.multiple_of(vlm_rows + s * ar, ar), ar))

    step = 32

    @pl.loop(0, vr // step)
    def _(i):
        o = pl.multiple_of(i * step, step)
        tok[pl.ds(pl.multiple_of((p * mp_size + m) * vr + o, step), step), :] = normalize(
            vlm_ref[pl.ds(o, step), :], gain_ref[...])

    @pl.loop(0, ar // step)
    def _(i):
        o = pl.multiple_of(i * step, step)
        tok[pl.ds(pl.multiple_of(vlm_rows + (p * mp_size + m) * ar + o, step), step), :] = normalize(
            act_ref[pl.ds(o, step), :], gain_ref[...])

    def tok_copy(pp, mm, part, to, slot):
        rows = token_rows(pp, mm)[part]
        return pltpu.make_async_remote_copy(
            src_ref=tok.at[rows, :], dst_ref=tok.at[rows, :], send_sem=tok_send,
            recv_sem=tok_recv.at[slot, 0 if slot == 3 else part], device_id=to, device_id_type=MESH)

    m_y = (1 - y) * 2 + c
    for part in (1, 0):
        tok_copy(p, m, part, xpart, 0).start()
        tok_copy(p, m, part, ypart, 1).start()
    for part in (1, 0):
        tok_copy(p, m, part, sibling, 3).start()

    def far_token_copy(part, c_from):
        rows = token_rows(p, m)[part]
        at = pl.ds(pl.multiple_of(c_from * (vr + ar) + part * vr, math.gcd(vr, ar)), (vr, ar)[part])
        return pltpu.make_async_remote_copy(
            src_ref=tok.at[rows, :], dst_ref=far_tok.at[at, :], send_sem=ft_send, recv_sem=ft_recv,
            device_id=(inward * 2 + p, y * 2 + 1), device_id_type=MESH)

    if far:
        @pl.when(end)
        def _():
            for part in (0, 1):
                far_token_copy(part, c).start()

    def far_w_copy(panel, to, slot):
        at = far_w.at[:, pl.ds(pl.multiple_of(panel * width, width), width)]
        return pltpu.make_async_remote_copy(
            src_ref=at if slot == 3 else wbuf.at[:, chunk(0)], dst_ref=at, send_sem=fw_send, recv_sem=fw_recv.at[slot],
            device_id=to, device_id_type=MESH)

    def spread_far_w():
        @pl.when(near & (c == 0))
        def _():
            far_w_copy(y * 2 + p, (g * 2 + 1 - p, y * 2 + 1), 1).start()
            far_w_copy(y * 2 + p, (d, (1 - y) * 2 + 1), 2).start()
            far_w_copy(y * 2 + p, sibling, 0).start()

    def relay_far_w():
        @pl.when(near & (c == 1))
        def _():
            far_w_copy(y * 2 + 1 - p, ypart, 1).wait_recv()
            far_w_copy(y * 2 + 1 - p, ypart, 3).start()

    def far_hid_copies(same_chip):
        for c_from in (0, 1):
            base = c_from * (vr + ar)
            m_from = y * 2 + c_from
            for step_y in (0, 1):
                y_to = y if step_y == 0 else 1 - y
                for step_p in (0, 1):
                    b = p if step_p == 0 else 1 - p
                    cols_at = pl.ds(pl.multiple_of((y_to * 2 + b) * width, width), width)
                    if (step_y == 0 and step_p == 0) == same_chip:
                        yield pltpu.make_async_remote_copy(
                            src_ref=far_hid.at[pl.ds(base, vr), cols_at],
                            dst_ref=vlm_out.at[pl.ds(pl.multiple_of((p * mp_size + m_from) * vr, vr), vr), chunk(0)],
                            send_sem=fh_send, recv_sem=fh_recv, device_id=(toward * 2 + b, y_to * 2), device_id_type=MESH)
                    if (step_y == 0) == same_chip:
                        yield pltpu.make_async_remote_copy(
                            src_ref=far_hid.at[pl.ds(base + vr, ar), cols_at],
                            dst_ref=act_out.at[pl.ds(pl.multiple_of(m_from * ar, ar), ar), out_cols(b, chunk(0))],
                            send_sem=fh_send, recv_sem=fh_recv, device_id=(toward * 2 + p, y_to * 2), device_id_type=MESH)

    def far_compute():
        @pl.when(near & (c == 1))
        def _():
            pltpu.make_async_remote_copy(
                src_ref=far_tok, dst_ref=far_tok, send_sem=ft_send, recv_sem=ft_recv,
                device_id=sibling, device_id_type=MESH).wait_recv()
            far_w_copy(y * 2, sibling, 0).wait_recv()
            far_w_copy(y * 2, sibling, 2).wait_recv()
            far_w_copy(y * 2, sibling, 3).wait_recv()

            @pl.loop(0, 2)
            def _(i):
                rows = pl.ds(pl.multiple_of(i * (vr + ar), math.gcd(vr, ar)), vr + ar)

                @pl.loop(0, 2)
                def _(j):
                    at = pl.ds(pl.multiple_of(j * 2 * width, width), 2 * width)
                    pre = jnp.dot(far_tok[rows, :], far_w[:, at], preferred_element_type=jnp.float32)
                    far_hid[rows, at] = gelu(pre)

            for copy in far_hid_copies(True):
                copy.start()

    def relay_first():
        tok_copy(1 - p, m, 1, sibling, 0).wait_recv()
        tok_copy(1 - p, m, 1, ypart, 2).start()
        tok_copy(p, m_y, 1, sibling, 1).wait_recv()
        tok_copy(p, m_y, 0, sibling, 1).wait_recv()
        tok_copy(p, m_y, 0, xpart, 2).start()
        tok_copy(1 - p, m, 0, sibling, 0).wait_recv()
        for part in (1, 0):
            tok_copy(1 - p, m, part, sibling, 3).start()
            tok_copy(p, m_y, part, sibling, 3).start()

    def relay_second():
        for part in (0, 1):
            tok_copy(1 - p, m_y, part, sibling, 2).wait_recv()
            tok_copy(1 - p, m_y, part, sibling, 3).start()

    def all_tokens():
        count = mp_size * (vr + ar)
        there = tok.at[pl.ds(0, count), :]
        pltpu.make_async_remote_copy(
            src_ref=there, dst_ref=there, send_sem=tok_send, recv_sem=tok_recv.at[3, 0],
            device_id=sibling, device_id_type=MESH).wait_recv()

    ex = pltpu.make_async_remote_copy(
        src_ref=wbuf.at[pl.ds(pl.multiple_of(g * r + (1 - p) * half, half), half), :],
        dst_ref=new_out.at[:, pl.ds(pl.multiple_of(p * cols, cols), cols)],
        send_sem=ex_send, recv_sem=ex_recv, device_id=xpart, device_id_type=MESH)
    kept = pltpu.make_async_copy(
        wbuf.at[pl.ds(pl.multiple_of(g * r + p * half, half), half), :],
        new_out.at[:, pl.ds(pl.multiple_of(p * cols, cols), cols)], loc_sem.at[0])

    def arrive_at(t, i):
        k = t - i
        inside = (k >= 0) & (k < n) & jnp.logical_not(short & (k == 0))

        @pl.when(inside & (g - 1 - i >= 0))
        def _():
            w_arrival(g - 1 - i, k).wait_recv()
            send_w(g - 1 - i, k, 1)

        @pl.when(inside & (g + 1 + i < groups))
        def _():
            w_arrival(g + 1 + i, k).wait_recv()
            send_w(g + 1 + i, k, 0)

    def send_next(t):
        for side in (0, 1):
            ahead = jnp.where(brief[side] & (t < 2), 4, jnp.where(last[side] & (t >= 2), 1, 2))
            k = jnp.where(last[side] & (t == n - 1), t, t + ahead)
            pause = last[side] & ((t == 2) | (t == n - 2)) | brief[side] & (t >= 2) & (t < n - 3)

            @pl.when((k < n) & jnp.logical_not(end) & jnp.logical_not(pause))
            def _():
                send_w(g, k, side)

    def arrive_far(t):
        arrive_at(t, groups - 2)

    def arrive_near(t):
        @pl.loop(0, groups - 3)
        def _(i):
            arrive_at(t, groups - 3 - i)

        held = end & far & (t >= n - 1)

        @pl.when(jnp.logical_not(held))
        def _():
            arrive_at(t, 0)

        if t == n:
            @pl.when(held)
            def _():
                arrive_at(n - 1, 0)

        send_next(t)

    def arrive(t):
        @pl.loop(0, groups - 1)
        def _(i):
            arrive_at(t, i)

        send_next(t)

    tile = math.gcd(256, math.gcd(vlm_rows, act_rows))
    a_tiles, v_tiles = act_rows // tile, vlm_rows // tile

    def out_cols(side, cc):
        return pl.ds(pl.multiple_of(side * cols + cc.start, width), cc.size)

    def tile_rows(start):
        return pl.ds(pl.multiple_of(start, tile), tile)

    def hid_copy(cc, t):
        return pltpu.make_async_remote_copy(
            src_ref=hid.at[tile_rows(vlm_rows + (1 - p) * act_rows + t * tile), cc],
            dst_ref=act_out.at[tile_rows(t * tile), out_cols(p, cc)],
            send_sem=hid_send, recv_sem=hid_recv, device_id=xpart, device_id_type=MESH)

    def own_copy(cc):
        return pltpu.make_async_copy(
            hid.at[pl.ds(pl.multiple_of(vlm_rows + p * act_rows, act_rows), act_rows), cc],
            act_out.at[:, out_cols(p, cc)], loc_sem.at[1])

    def vlm_copy(cc):
        return pltpu.make_async_copy(hid.at[pl.ds(0, vlm_rows), cc], vlm_out.at[:, cc], loc_sem.at[2])

    def hidden(rows, cc):
        pre = jnp.dot(tok[rows, :], wbuf[:, cc], preferred_element_type=jnp.float32)
        hid[rows, cc] = gelu(pre)

    def for_partner(cc):
        @pl.loop(0, a_tiles)
        def _(t):
            hidden(tile_rows(vlm_rows + (1 - p) * act_rows + t * tile), cc)
            hid_copy(cc, t).start()

    def for_self(cc):
        @pl.loop(0, a_tiles + v_tiles)
        def _(t):
            hidden(tile_rows(jnp.where(
                t < a_tiles, vlm_rows + p * act_rows + t * tile, (t - a_tiles) * tile)), cc)

    warm = groups - 1

    @pl.loop(0, warm)
    def _(t):
        arrive(t)

    relay_first()
    if far:
        spread_far_w()

    @pl.when(jnp.logical_not(near))
    def _():
        ex.start()

    kept.start()
    arrive(warm)
    arrive(warm + 1)
    relay_second()
    arrive(warm + 2)
    if far:
        relay_far_w()

    @pl.when(near)
    def _():
        ex.start()

    all_tokens()

    def pair_at(j, body):
        if far and j == 0:
            @pl.when(short)
            def _():
                body(chunk(1))

            @pl.when(jnp.logical_not(short))
            def _():
                body(chunk(0, 2))
        else:
            body(chunk(j, 2))

    for j in range(0, 4, 2):
        pair_at(j, for_partner)
    for j in range(0, 4, 2):
        pair_at(j, for_self)
    for j in range(4, n):
        arrive_far(warm + j - 1)
        if far and j == n - 1:
            far_compute()
        for_partner(chunk(j))
        arrive_near(warm + j - 1)
        if j % 2 == 1:
            for_self(chunk(j - 1, 2))

    tail_cols, all_cols = chunk(1, n - 1), chunk(0, n)

    def by_width(brief, body):
        @pl.when(brief)
        def _():
            body(tail_cols)

        @pl.when(jnp.logical_not(brief))
        def _():
            body(all_cols)

    def copy_out(cc):
        own_copy(cc).start()
        vlm_copy(cc).start()

    def copied_out(cc):
        own_copy(cc).wait()
        vlm_copy(cc).wait()

    by_width(short, copy_out)

    def w_sent(block, side):
        for skip in (0, 1):
            for fewer in (0, late):
                few = w_last(block, side)

                @pl.when((brief[side] if skip else jnp.logical_not(brief[side])) & (few if fewer else jnp.logical_not(few)))
                def _():
                    w_copy(block, chunk(0, n - skip - fewer), w_slot(block, side), ex_recv, side).wait_send()

    @pl.loop(0, groups)
    def _(block):
        @pl.when(has_left & (block >= g))
        def _():
            w_sent(block, 0)

        @pl.when(has_right & (block <= g))
        def _():
            w_sent(block, 1)

    def bytes_of(ref, send, recv):
        return pltpu.make_async_remote_copy(
            src_ref=ref, dst_ref=ref, send_sem=send, recv_sem=recv, device_id=sibling, device_id_type=MESH)

    if far:
        @pl.when(near & (c == 1))
        def _():
            for copy in far_hid_copies(False):
                copy.start()
            bytes_of(far_w.at[:, pl.ds(0, width)], fw_send, ex_recv).wait_send()
            bytes_of(hid.at[pl.ds(0, 8 * (vr + ar)), chunk(0)], fh_send, ex_recv).wait_send()

        @pl.when(near & (c == 0))
        def _():
            bytes_of(wbuf.at[:, pl.ds(0, 3 * width)], fw_send, ex_recv).wait_send()

        @pl.when(near)
        def _():
            bytes_of(wbuf.at[pl.ds(0, r), chunk(0, late)], w_send.at[groups + 1], ex_recv).wait_send()

        @pl.when(end)
        def _():
            bytes_of(tok.at[pl.ds(0, vr + ar), :], ft_send, ex_recv).wait_send()

    bytes_of(tok.at[pl.ds(0, 7 * (vr + ar)), :], tok_send, ex_recv).wait_send()
    ex.wait_send()
    taken = new_out.at[:, pl.ds(pl.multiple_of((1 - p) * cols, cols), cols)]
    bytes_of(taken, ex_send, ex_recv).wait_recv()
    kept.wait()

    def exchanged(cc):
        there = act_out.at[:, out_cols(1 - p, cc)]
        bytes_of(there, hid_send, hid_recv).wait_send()
        bytes_of(there, hid_send, hid_recv).wait_recv()

    by_width(short, copied_out)
    by_width(short, exchanged)
    if far:
        @pl.when(short)
        def _():
            bytes_of(hid.at[:, chunk(0)], fh_send, fh_recv).wait_recv()


def store(*refs):
    count = (len(refs) - 1) // 2
    copies = [pltpu.make_async_copy(refs[i], refs[count + i], refs[-1].at[i]) for i in range(count)]
    for copy in copies:
        copy.start()
    for copy in copies:
        copy.wait()


def solution(mesh):
    groups, mp_size = mesh.shape["dp"] // 2, mesh.shape["mp"]

    def local(vlm_tokens, action_tokens, norm_gain, proj_old):
        vr, ar = vlm_tokens.shape[0], action_tokens.shape[0]
        features = vlm_tokens.shape[1]
        r, cols = proj_old.shape
        vlm_rows, act_rows = 2 * mp_size * vr, mp_size * ar
        bf16 = jnp.bfloat16
        dma = pltpu.SemaphoreType.DMA
        hbm, anywhere = pl.BlockSpec(memory_space=pltpu.HBM), pl.BlockSpec(memory_space=pl.ANY)
        chunks = cols // chunk_width(cols)
        shapes = (
            jax.ShapeDtypeStruct((vlm_rows, cols), bf16),
            jax.ShapeDtypeStruct((act_rows, 2 * cols), bf16),
            jax.ShapeDtypeStruct((r // 2, 2 * cols), bf16),
        )
        results = pl.pallas_call(
            functools.partial(kernel, groups, mp_size),
            name="up_gelu",
            out_shape=shapes,
            in_specs=[hbm] * 4,
            out_specs=(anywhere,) * 3,
            scratch_shapes=[
                pltpu.VMEM((vr, features), bf16),
                pltpu.VMEM((ar, features), bf16),
                pltpu.VMEM((1, features), jnp.float32),
                pltpu.VMEM((vlm_rows + 2 * act_rows, features), bf16),
                pltpu.VMEM((groups * r, cols), bf16),
                pltpu.VMEM((vlm_rows + 2 * act_rows, cols), bf16),
                dma, dma((4, 2)), dma((groups + 2,)), dma((groups - 1, chunks)), dma, dma, dma, dma, dma((4,)), dma((3,)),
                pltpu.VMEM((2 * (vr + ar), features), bf16),
                pltpu.VMEM((groups * r, 4 * chunk_width(cols)), bf16),
                pltpu.VMEM((2 * (vr + ar), 4 * chunk_width(cols)), bf16),
                dma, dma, dma, dma((4,)), dma, dma, pltpu.SemaphoreType.REGULAR,
            ],
            compiler_params=pltpu.CompilerParams(
                collective_id=0, has_side_effects=True, vmem_limit_bytes=48 * 1024 * 1024),
        )(*[pltpu.with_memory_space_constraint(array, pltpu.HBM) for array in (
            vlm_tokens, action_tokens, norm_gain.reshape(1, -1), proj_old)])
        return pl.pallas_call(
            store,
            name="store",
            out_shape=shapes,
            in_specs=[anywhere] * 3,
            out_specs=(hbm,) * 3,
            scratch_shapes=[dma((3,))],
            compiler_params=pltpu.CompilerParams(vmem_limit_bytes=1024 * 1024),
        )(*results)

    return jax.shard_map(
        local,
        mesh=mesh,
        in_specs=(P(("dp", "mp"), None), P(("dp", "mp"), None), P(), P("dp", "mp")),
        out_specs=(P("dp", "mp"), P("dp", "mp"), P("dp", "mp")),
        check_vma=False,
    )
```

```python
import functools
import math
import jax
import jax.numpy as jnp
from jax import lax
from jax.experimental import pallas as pl
from jax.experimental.pallas import tpu as pltpu
from jax.sharding import PartitionSpec as P

MESH = pl.DeviceIdType.MESH
epsilon = 1e-06


def normalize(row_values, norm_gain):
    values = row_values.astype(jnp.float32)
    factor = lax.rsqrt(jnp.mean(values * values, axis=-1, keepdims=True) + epsilon)
    return (values * factor * norm_gain).astype(jnp.bfloat16)


def gelu(u):
    return (u * 0.5 * (1.0 + lax.erf(u * math.sqrt(0.5)))).astype(jnp.bfloat16)


def chunk_width(cols):
    return max(cols // 8, 128)


def kernel(groups, mp_size, vlm_hbm, act_hbm, gain_hbm, proj_hbm, vlm_out, act_out, new_out,
           vlm_ref, act_ref, gain_ref, tok, wbuf, hid, tok_send, tok_recv, w_send, w_recv, ex_send, ex_recv,
           hid_send, hid_recv, load_sem, loc_sem, far_tok, far_w, far_hid, ft_send, ft_recv, fw_send, fw_recv,
           fh_send, fh_recv, ready):
    d = lax.axis_index("dp")
    m = lax.axis_index("mp")
    g, p = d // 2, d % 2
    y, c = m // 2, m % 2
    vr, ar = vlm_ref.shape[0], act_ref.shape[0]
    r, cols = proj_hbm.shape
    half = r // 2
    width = chunk_width(cols)
    n = cols // width
    vlm_rows, act_rows = 2 * mp_size * vr, mp_size * ar
    sibling = (d, y * 2 + 1 - c)
    xpart = (g * 2 + 1 - p, m)
    ypart = (d, (1 - y) * 2 + c)
    has_left, has_right = g > 0, g < groups - 1
    far = groups >= 4 and n >= 8
    late = 2
    end = (g == 0) | (g == groups - 1)
    near = ((g == 1) | (g == groups - 2)) & far
    short = end & (c == 0) & far
    toward = jnp.where(g <= 1, 0, groups - 1)
    inward = jnp.where(g == 0, 1, groups - 2)

    def chunk(k, count=1):
        return pl.ds(pl.multiple_of(k * width, width), count * width)

    def block_rows(block):
        return pl.ds(pl.multiple_of(block * r, r), r)

    barrier = pltpu.get_barrier_semaphore()

    left, right = (d - 2, m), (d + 2, m)
    earlier = ((has_left, left), (p == 1, xpart), (y == 1, ypart), (c == 1, sibling))
    later = ((has_right, right), (p == 0, xpart), (y == 0, ypart), (c == 0, sibling))

    def number(flags):
        return sum(flag.astype(jnp.int32) for flag in flags)

    def greet(semaphore, others):
        for flag, other in others:
            @pl.when(flag)
            def _():
                pl.semaphore_signal(semaphore, inc=1, device_id=other, device_id_type=MESH)

    greet(barrier, later + ((near & (c == 1), (toward * 2 + p, y * 2)),))
    w_load = pltpu.make_async_copy(proj_hbm, wbuf.at[block_rows(g), :], load_sem.at[3])
    loads = [pltpu.make_async_copy(src, dst, load_sem.at[i]) for i, (src, dst) in enumerate(
        ((gain_hbm, gain_ref), (vlm_hbm, vlm_ref), (act_hbm, act_ref)))]
    for load in loads:
        load.start()
    w_load.start()
    pl.semaphore_wait(barrier, number([flag for flag, _ in earlier] + [short]))
    greet(ready, earlier)

    brief = (near & (g == 1) & (c == 0), near & (g == groups - 2) & (c == 0))
    last = (near & (g == 1), near & (g == groups - 2))

    def w_copy(block, cc, send, recv, side, from_hbm=False):
        there = wbuf.at[block_rows(block), cc]
        return pltpu.make_async_remote_copy(
            src_ref=proj_hbm.at[:, cc] if from_hbm else there,
            dst_ref=there,
            send_sem=w_send.at[send],
            recv_sem=recv,
            device_id=left if side == 0 else right,
            device_id_type=MESH,
        )

    def w_slot(block, side):
        return jnp.where((block == g) & (side == 0), groups, block)

    def w_last(block, side):
        return last[side] & (block == (groups - 1 if side == 0 else 0))

    def w_chunk(block, k, side, from_hbm=False):
        return w_copy(
            block, chunk(k), jnp.where(w_last(block, side) & (k >= n - late), groups + 1, w_slot(block, side)),
            w_recv.at[lax.rem(block - g + 2 * groups + (0 if side == 0 else -2), groups), k], side, from_hbm)

    def w_arrival(block, k):
        there = wbuf.at[block_rows(block), chunk(k)]
        return pltpu.make_async_remote_copy(
            src_ref=there, dst_ref=there, send_sem=w_send.at[block],
            recv_sem=w_recv.at[lax.rem(block - g + 2 * groups - 1, groups), k],
            device_id=sibling, device_id_type=MESH)

    def send_w(block, k, side, from_hbm=False):
        ok = has_left if side == 0 else has_right

        @pl.when(ok & jnp.logical_not(brief[side] & (k == 0)))
        def _():
            w_chunk(block, k, side, from_hbm).start()

    def send_own(k):
        send_w(g, k, 0)
        send_w(g, k, 1)

    for k in (0, 1):
        send_w(g, k, 0, True)
    answers = number([flag for flag, _ in later])

    @pl.when(answers > 0)
    def _():
        pl.semaphore_wait(ready, answers)

    for k in (0, 1):
        send_w(g, k, 1, True)
    w_load.wait()
    for side in (0, 1):
        @pl.when(brief[side])
        def _():
            for k in (2, 3):
                send_w(g, k, side)


    @pl.when(end)
    def _():
        @pl.loop(2, n)
        def _(k):
            send_own(k)

    for load in loads:
        load.wait()

    def token_rows(pp, mm):
        s = pp * mp_size + mm
        return (pl.ds(pl.multiple_of(s * vr, vr), vr), pl.ds(pl.multiple_of(vlm_rows + s * ar, ar), ar))

    step = 32

    @pl.loop(0, vr // step)
    def _(i):
        o = pl.multiple_of(i * step, step)
        tok[pl.ds(pl.multiple_of((p * mp_size + m) * vr + o, step), step), :] = normalize(
            vlm_ref[pl.ds(o, step), :], gain_ref[...])

    @pl.loop(0, ar // step)
    def _(i):
        o = pl.multiple_of(i * step, step)
        tok[pl.ds(pl.multiple_of(vlm_rows + (p * mp_size + m) * ar + o, step), step), :] = normalize(
            act_ref[pl.ds(o, step), :], gain_ref[...])

    def tok_copy(pp, mm, part, to, slot):
        rows = token_rows(pp, mm)[part]
        return pltpu.make_async_remote_copy(
            src_ref=tok.at[rows, :], dst_ref=tok.at[rows, :], send_sem=tok_send,
            recv_sem=tok_recv.at[slot, 0 if slot == 3 else part], device_id=to, device_id_type=MESH)

    m_y = (1 - y) * 2 + c
    for part in (1, 0):
        tok_copy(p, m, part, xpart, 0).start()
        tok_copy(p, m, part, ypart, 1).start()
    for part in (1, 0):
        tok_copy(p, m, part, sibling, 3).start()

    def far_token_copy(part, c_from):
        rows = token_rows(p, m)[part]
        at = pl.ds(pl.multiple_of(c_from * ar + 2 * vr if part else c_from * vr, math.gcd(vr, ar)), (vr, ar)[part])
        return pltpu.make_async_remote_copy(
            src_ref=tok.at[rows, :], dst_ref=far_tok.at[at, :], send_sem=ft_send, recv_sem=ft_recv,
            device_id=(inward * 2 + p, y * 2 + 1), device_id_type=MESH)

    if far:
        @pl.when(end)
        def _():
            for part in (0, 1):
                far_token_copy(part, c).start()

    def far_w_copy(panel, to, slot):
        at = far_w.at[:, pl.ds(pl.multiple_of(panel * width, width), width)]
        return pltpu.make_async_remote_copy(
            src_ref=at if slot == 3 else wbuf.at[:, chunk(0)], dst_ref=at, send_sem=fw_send, recv_sem=fw_recv.at[slot],
            device_id=to, device_id_type=MESH)

    def spread_far_w():
        @pl.when(near & (c == 0))
        def _():
            far_w_copy(y * 2 + p, (g * 2 + 1 - p, y * 2 + 1), 1).start()
            far_w_copy(y * 2 + p, (d, (1 - y) * 2 + 1), 2).start()
            far_w_copy(y * 2 + p, sibling, 0).start()

    def relay_far_w():
        @pl.when(near & (c == 1))
        def _():
            far_w_copy(y * 2 + 1 - p, ypart, 1).wait_recv()
            far_w_copy(y * 2 + 1 - p, ypart, 3).start()

    def far_hid_copies(phase):
        for step_y in (0, 1):
            y_to = y if step_y == 0 else 1 - y
            for step_p in (0, 1):
                b = p if step_p == 0 else 1 - p
                cols_at = pl.ds(pl.multiple_of((y_to * 2 + b) * width, width), width)
                if 1 + step_y == phase:
                    yield pltpu.make_async_remote_copy(
                        src_ref=far_hid.at[pl.ds(2 * vr, 2 * ar), cols_at],
                        dst_ref=act_out.at[pl.ds(pl.multiple_of(y * 2 * ar, 2 * ar), 2 * ar), out_cols(b, chunk(0))],
                        send_sem=fh_send, recv_sem=fh_recv, device_id=(toward * 2 + p, y_to * 2), device_id_type=MESH)
                if (0 if step_p else 1 + step_y) == phase:
                    yield pltpu.make_async_remote_copy(
                        src_ref=far_hid.at[pl.ds(0, 2 * vr), cols_at],
                        dst_ref=vlm_out.at[pl.ds(pl.multiple_of((p * mp_size + y * 2) * vr, 2 * vr), 2 * vr), chunk(0)],
                        send_sem=fh_send, recv_sem=fh_recv, device_id=(toward * 2 + b, y_to * 2), device_id_type=MESH)

    def far_compute():
        @pl.when(near & (c == 1))
        def _():
            pltpu.make_async_remote_copy(
                src_ref=far_tok, dst_ref=far_tok, send_sem=ft_send, recv_sem=ft_recv,
                device_id=sibling, device_id_type=MESH).wait_recv()
            far_w_copy(y * 2, sibling, 0).wait_recv()
            far_w_copy(y * 2, sibling, 2).wait_recv()
            far_w_copy(y * 2, sibling, 3).wait_recv()

            @pl.loop(0, 2)
            def _(i):
                rows = pl.ds(pl.multiple_of(i * (vr + ar), math.gcd(vr, ar)), vr + ar)

                @pl.loop(0, 2)
                def _(j):
                    at = pl.ds(pl.multiple_of(j * 2 * width, width), 2 * width)
                    pre = jnp.dot(far_tok[rows, :], far_w[:, at], preferred_element_type=jnp.float32)
                    far_hid[rows, at] = gelu(pre)

            for copy in far_hid_copies(0):
                copy.start()

    def relay_first():
        tok_copy(1 - p, m, 1, sibling, 0).wait_recv()
        tok_copy(1 - p, m, 1, ypart, 2).start()
        tok_copy(p, m_y, 1, sibling, 1).wait_recv()
        tok_copy(p, m_y, 0, sibling, 1).wait_recv()
        tok_copy(p, m_y, 0, xpart, 2).start()
        tok_copy(1 - p, m, 0, sibling, 0).wait_recv()
        for part in (1, 0):
            tok_copy(1 - p, m, part, sibling, 3).start()
            tok_copy(p, m_y, part, sibling, 3).start()

    def relay_second():
        for part in (0, 1):
            tok_copy(1 - p, m_y, part, sibling, 2).wait_recv()
            tok_copy(1 - p, m_y, part, sibling, 3).start()

    def all_tokens():
        count = mp_size * (vr + ar)
        there = tok.at[pl.ds(0, count), :]
        pltpu.make_async_remote_copy(
            src_ref=there, dst_ref=there, send_sem=tok_send, recv_sem=tok_recv.at[3, 0],
            device_id=sibling, device_id_type=MESH).wait_recv()

    ex = pltpu.make_async_remote_copy(
        src_ref=wbuf.at[pl.ds(pl.multiple_of(g * r + (1 - p) * half, half), half), :],
        dst_ref=new_out.at[:, pl.ds(pl.multiple_of(p * cols, cols), cols)],
        send_sem=ex_send, recv_sem=ex_recv, device_id=xpart, device_id_type=MESH)
    kept = pltpu.make_async_copy(
        wbuf.at[pl.ds(pl.multiple_of(g * r + p * half, half), half), :],
        new_out.at[:, pl.ds(pl.multiple_of(p * cols, cols), cols)], loc_sem.at[0])

    def arrive_at(t, i):
        k = t - i
        inside = (k >= 0) & (k < n) & jnp.logical_not(short & (k == 0))

        @pl.when(inside & (g - 1 - i >= 0))
        def _():
            w_arrival(g - 1 - i, k).wait_recv()
            send_w(g - 1 - i, k, 1)

        @pl.when(inside & (g + 1 + i < groups))
        def _():
            w_arrival(g + 1 + i, k).wait_recv()
            send_w(g + 1 + i, k, 0)

    def send_next(t):
        for side in (0, 1):
            ahead = jnp.where(brief[side] & (t < 2), 4, jnp.where(last[side] & (t >= 2), 1, 2))
            k = jnp.where(last[side] & (t == n - 1), t, t + ahead)
            pause = last[side] & ((t == 2) | (t == n - 2)) | brief[side] & (t >= 2) & (t < n - 3)

            @pl.when((k < n) & jnp.logical_not(end) & jnp.logical_not(pause))
            def _():
                send_w(g, k, side)

    def arrive_far(t):
        arrive_at(t, groups - 2)

    def arrive_near(t):
        @pl.loop(0, groups - 3)
        def _(i):
            arrive_at(t, groups - 3 - i)

        held = end & far & (t >= n - 1)

        @pl.when(jnp.logical_not(held))
        def _():
            arrive_at(t, 0)

        if t == n:
            @pl.when(held)
            def _():
                arrive_at(n - 1, 0)

        send_next(t)

    def arrive(t):
        @pl.loop(0, groups - 1)
        def _(i):
            arrive_at(t, i)

        send_next(t)

    tile = math.gcd(256, math.gcd(vlm_rows, act_rows))
    a_tiles, v_tiles = act_rows // tile, vlm_rows // tile

    def out_cols(side, cc):
        return pl.ds(pl.multiple_of(side * cols + cc.start, width), cc.size)

    def tile_rows(start):
        return pl.ds(pl.multiple_of(start, tile), tile)

    def hid_copy(cc, t):
        return pltpu.make_async_remote_copy(
            src_ref=hid.at[tile_rows(vlm_rows + (1 - p) * act_rows + t * tile), cc],
            dst_ref=act_out.at[tile_rows(t * tile), out_cols(p, cc)],
            send_sem=hid_send, recv_sem=hid_recv, device_id=xpart, device_id_type=MESH)

    def own_copy(cc):
        return pltpu.make_async_copy(
            hid.at[pl.ds(pl.multiple_of(vlm_rows + p * act_rows, act_rows), act_rows), cc],
            act_out.at[:, out_cols(p, cc)], loc_sem.at[1])

    def vlm_copy(cc):
        return pltpu.make_async_copy(hid.at[pl.ds(0, vlm_rows), cc], vlm_out.at[:, cc], loc_sem.at[2])

    def hidden(rows, cc):
        pre = jnp.dot(tok[rows, :], wbuf[:, cc], preferred_element_type=jnp.float32)
        hid[rows, cc] = gelu(pre)

    def for_partner(cc):
        @pl.loop(0, a_tiles)
        def _(t):
            hidden(tile_rows(vlm_rows + (1 - p) * act_rows + t * tile), cc)
            hid_copy(cc, t).start()

    def for_self(cc):
        @pl.loop(0, a_tiles + v_tiles)
        def _(t):
            hidden(tile_rows(jnp.where(
                t < a_tiles, vlm_rows + p * act_rows + t * tile, (t - a_tiles) * tile)), cc)

    warm = groups - 1

    @pl.loop(0, warm)
    def _(t):
        arrive(t)

    relay_first()
    if far:
        spread_far_w()

    @pl.when(jnp.logical_not(near))
    def _():
        ex.start()

    kept.start()
    arrive(warm)
    arrive(warm + 1)
    relay_second()
    arrive(warm + 2)
    if far:
        relay_far_w()

    @pl.when(near)
    def _():
        ex.start()

    all_tokens()

    def pair_at(j, body):
        if far and j == 0:
            @pl.when(short)
            def _():
                body(chunk(1))

            @pl.when(jnp.logical_not(short))
            def _():
                body(chunk(0, 2))
        else:
            body(chunk(j, 2))

    for j in range(0, 4, 2):
        pair_at(j, for_partner)
    for j in range(0, 4, 2):
        pair_at(j, for_self)
    for j in range(4, n):
        arrive_far(warm + j - 1)
        if far and j == n - 2:
            far_compute()
        if far and j == n - 1:
            @pl.when(near & (c == 1))
            def _():
                for copy in far_hid_copies(1):
                    copy.start()

        for_partner(chunk(j))
        arrive_near(warm + j - 1)
        if j % 2 == 1:
            for_self(chunk(j - 1, 2))

    tail_cols, all_cols = chunk(1, n - 1), chunk(0, n)

    def by_width(brief, body):
        @pl.when(brief)
        def _():
            body(tail_cols)

        @pl.when(jnp.logical_not(brief))
        def _():
            body(all_cols)

    def copy_out(cc):
        own_copy(cc).start()
        vlm_copy(cc).start()

    def copied_out(cc):
        own_copy(cc).wait()
        vlm_copy(cc).wait()

    by_width(short, copy_out)

    def w_sent(block, side):
        for skip in (0, 1):
            for fewer in (0, late):
                few = w_last(block, side)

                @pl.when((brief[side] if skip else jnp.logical_not(brief[side])) & (few if fewer else jnp.logical_not(few)))
                def _():
                    w_copy(block, chunk(0, n - skip - fewer), w_slot(block, side), ex_recv, side).wait_send()

    if far:
        @pl.when(near & (c == 1))
        def _():
            for side in (0, 1):
                @pl.when(last[side])
                def _():
                    w_sent(groups - 1 if side == 0 else 0, side)

            for copy in far_hid_copies(2):
                copy.start()

    @pl.loop(0, groups)
    def _(block):
        @pl.when(has_left & (block >= g) & jnp.logical_not(w_last(block, 0) & (c == 1)))
        def _():
            w_sent(block, 0)

        @pl.when(has_right & (block <= g) & jnp.logical_not(w_last(block, 1) & (c == 1)))
        def _():
            w_sent(block, 1)

    def bytes_of(ref, send, recv):
        return pltpu.make_async_remote_copy(
            src_ref=ref, dst_ref=ref, send_sem=send, recv_sem=recv, device_id=sibling, device_id_type=MESH)

    if far:
        @pl.when(near & (c == 1))
        def _():
            bytes_of(far_w.at[:, pl.ds(0, width)], fw_send, ex_recv).wait_send()
            bytes_of(hid.at[pl.ds(0, 8 * (vr + ar)), chunk(0)], fh_send, ex_recv).wait_send()

        @pl.when(near & (c == 0))
        def _():
            bytes_of(wbuf.at[:, pl.ds(0, 3 * width)], fw_send, ex_recv).wait_send()

        @pl.when(near)
        def _():
            bytes_of(wbuf.at[pl.ds(0, r), chunk(0, late)], w_send.at[groups + 1], ex_recv).wait_send()

        @pl.when(end)
        def _():
            bytes_of(tok.at[pl.ds(0, vr + ar), :], ft_send, ex_recv).wait_send()

    bytes_of(tok.at[pl.ds(0, 7 * (vr + ar)), :], tok_send, ex_recv).wait_send()
    ex.wait_send()
    taken = new_out.at[:, pl.ds(pl.multiple_of((1 - p) * cols, cols), cols)]
    bytes_of(taken, ex_send, ex_recv).wait_recv()
    kept.wait()

    def exchanged(cc):
        there = act_out.at[:, out_cols(1 - p, cc)]
        bytes_of(there, hid_send, hid_recv).wait_send()
        bytes_of(there, hid_send, hid_recv).wait_recv()

    by_width(short, copied_out)
    by_width(short, exchanged)
    if far:
        @pl.when(short)
        def _():
            bytes_of(hid.at[:, chunk(0)], fh_send, fh_recv).wait_recv()


def store(*refs):
    count = (len(refs) - 1) // 2
    copies = [pltpu.make_async_copy(refs[i], refs[count + i], refs[-1].at[i]) for i in range(count)]
    for copy in copies:
        copy.start()
    for copy in copies:
        copy.wait()


def solution(mesh):
    groups, mp_size = mesh.shape["dp"] // 2, mesh.shape["mp"]

    def local(vlm_tokens, action_tokens, norm_gain, proj_old):
        vr, ar = vlm_tokens.shape[0], action_tokens.shape[0]
        features = vlm_tokens.shape[1]
        r, cols = proj_old.shape
        vlm_rows, act_rows = 2 * mp_size * vr, mp_size * ar
        bf16 = jnp.bfloat16
        dma = pltpu.SemaphoreType.DMA
        hbm, anywhere = pl.BlockSpec(memory_space=pltpu.HBM), pl.BlockSpec(memory_space=pl.ANY)
        chunks = cols // chunk_width(cols)
        shapes = (
            jax.ShapeDtypeStruct((vlm_rows, cols), bf16),
            jax.ShapeDtypeStruct((act_rows, 2 * cols), bf16),
            jax.ShapeDtypeStruct((r // 2, 2 * cols), bf16),
        )
        results = pl.pallas_call(
            functools.partial(kernel, groups, mp_size),
            name="up_gelu",
            out_shape=shapes,
            in_specs=[hbm] * 4,
            out_specs=(anywhere,) * 3,
            scratch_shapes=[
                pltpu.VMEM((vr, features), bf16),
                pltpu.VMEM((ar, features), bf16),
                pltpu.VMEM((1, features), jnp.float32),
                pltpu.VMEM((vlm_rows + 2 * act_rows, features), bf16),
                pltpu.VMEM((groups * r, cols), bf16),
                pltpu.VMEM((vlm_rows + 2 * act_rows, cols), bf16),
                dma, dma((4, 2)), dma((groups + 2,)), dma((groups - 1, chunks)), dma, dma, dma, dma, dma((4,)), dma((3,)),
                pltpu.VMEM((2 * (vr + ar), features), bf16),
                pltpu.VMEM((groups * r, 4 * chunk_width(cols)), bf16),
                pltpu.VMEM((2 * (vr + ar), 4 * chunk_width(cols)), bf16),
                dma, dma, dma, dma((4,)), dma, dma, pltpu.SemaphoreType.REGULAR,
            ],
            compiler_params=pltpu.CompilerParams(
                collective_id=0, has_side_effects=True, vmem_limit_bytes=48 * 1024 * 1024),
        )(*[pltpu.with_memory_space_constraint(array, pltpu.HBM) for array in (
            vlm_tokens, action_tokens, norm_gain.reshape(1, -1), proj_old)])
        return pl.pallas_call(
            store,
            name="store",
            out_shape=shapes,
            in_specs=[anywhere] * 3,
            out_specs=(hbm,) * 3,
            scratch_shapes=[dma((3,))],
            compiler_params=pltpu.CompilerParams(vmem_limit_bytes=1024 * 1024),
        )(*results)

    return jax.shard_map(
        local,
        mesh=mesh,
        in_specs=(P(("dp", "mp"), None), P(("dp", "mp"), None), P(), P("dp", "mp")),
        out_specs=(P("dp", "mp"), P("dp", "mp"), P("dp", "mp")),
        check_vma=False,
    )
```

```python
import functools
import math
import jax
import jax.numpy as jnp
from jax import lax
from jax.experimental import pallas as pl
from jax.experimental.pallas import tpu as pltpu
from jax.sharding import PartitionSpec as P

MESH = pl.DeviceIdType.MESH
epsilon = 1e-06


def normalize(row_values, norm_gain):
    values = row_values.astype(jnp.float32)
    factor = lax.rsqrt(jnp.mean(values * values, axis=-1, keepdims=True) + epsilon)
    return (values * factor * norm_gain).astype(jnp.bfloat16)


def gelu(u):
    return (u * 0.5 * (1.0 + lax.erf(u * math.sqrt(0.5)))).astype(jnp.bfloat16)


def chunk_width(cols):
    return max(cols // 8, 128)


def kernel(groups, mp_size, vlm_hbm, act_hbm, gain_hbm, proj_hbm, vlm_out, act_out, new_out,
           vlm_ref, act_ref, gain_ref, tok, wbuf, hid, tok_send, tok_recv, w_send, w_recv, ex_send, ex_recv,
           hid_send, hid_recv, load_sem, loc_sem, far_tok, far_w, far_hid, ft_send, ft_recv, fw_send, fw_recv,
           fh_send, fh_recv, ready):
    d = lax.axis_index("dp")
    m = lax.axis_index("mp")
    g, p = d // 2, d % 2
    y, c = m // 2, m % 2
    vr, ar = vlm_ref.shape[0], act_ref.shape[0]
    r, cols = proj_hbm.shape
    half = r // 2
    width = chunk_width(cols)
    n = cols // width
    vlm_rows, act_rows = 2 * mp_size * vr, mp_size * ar
    sibling = (d, y * 2 + 1 - c)
    xpart = (g * 2 + 1 - p, m)
    ypart = (d, (1 - y) * 2 + c)
    has_left, has_right = g > 0, g < groups - 1
    far = groups >= 4 and n >= 8
    late = 2
    end = (g == 0) | (g == groups - 1)
    near = ((g == 1) | (g == groups - 2)) & far
    short = end & (c == 0) & far
    toward = jnp.where(g <= 1, 0, groups - 1)
    inward = jnp.where(g == 0, 1, groups - 2)

    def chunk(k, count=1):
        return pl.ds(pl.multiple_of(k * width, width), count * width)

    def block_rows(block):
        return pl.ds(pl.multiple_of(block * r, r), r)

    barrier = pltpu.get_barrier_semaphore()

    left, right = (d - 2, m), (d + 2, m)
    leads = ((g == 0) & (c == 0)) | ((g > 0) & (c == 1))
    earlier = ((has_left, left), (p == 1, xpart), (y == 1, ypart), (jnp.logical_not(leads), sibling))
    later = ((has_right, right), (p == 0, xpart), (y == 0, ypart), (leads, sibling))

    def number(flags):
        return sum(flag.astype(jnp.int32) for flag in flags)

    def greet(semaphore, others):
        for flag, other in others:
            @pl.when(flag)
            def _():
                pl.semaphore_signal(semaphore, inc=1, device_id=other, device_id_type=MESH)

    greet(barrier, later + ((near & (c == 1), (toward * 2 + p, y * 2)),))
    w_load = pltpu.make_async_copy(proj_hbm, wbuf.at[block_rows(g), :], load_sem.at[3])
    loads = [pltpu.make_async_copy(src, dst, load_sem.at[i]) for i, (src, dst) in enumerate(
        ((gain_hbm, gain_ref), (vlm_hbm, vlm_ref), (act_hbm, act_ref)))]
    for load in loads:
        load.start()
    w_load.start()
    pl.semaphore_wait(barrier, number([flag for flag, _ in earlier] + [short]))
    greet(ready, earlier)

    brief = (near & (g == 1) & (c == 0), near & (g == groups - 2) & (c == 0))
    last = (near & (g == 1), near & (g == groups - 2))

    def w_copy(block, cc, send, recv, side, from_hbm=False):
        there = wbuf.at[block_rows(block), cc]
        return pltpu.make_async_remote_copy(
            src_ref=proj_hbm.at[:, cc] if from_hbm else there,
            dst_ref=there,
            send_sem=w_send.at[send],
            recv_sem=recv,
            device_id=left if side == 0 else right,
            device_id_type=MESH,
        )

    def w_slot(block, side):
        return jnp.where((block == g) & (side == 0), groups, block)

    def w_last(block, side):
        return last[side] & (block == (groups - 1 if side == 0 else 0))

    def w_chunk(block, k, side, from_hbm=False):
        return w_copy(
            block, chunk(k), jnp.where(w_last(block, side) & (k >= n - late), groups + 1, w_slot(block, side)),
            w_recv.at[lax.rem(block - g + 2 * groups + (0 if side == 0 else -2), groups), k], side, from_hbm)

    def w_arrival(block, k):
        there = wbuf.at[block_rows(block), chunk(k)]
        return pltpu.make_async_remote_copy(
            src_ref=there, dst_ref=there, send_sem=w_send.at[block],
            recv_sem=w_recv.at[lax.rem(block - g + 2 * groups - 1, groups), k],
            device_id=sibling, device_id_type=MESH)

    def send_w(block, k, side, from_hbm=False):
        ok = has_left if side == 0 else has_right

        @pl.when(ok & jnp.logical_not(brief[side] & (k == 0)))
        def _():
            w_chunk(block, k, side, from_hbm).start()

    def send_own(k):
        send_w(g, k, 0)
        send_w(g, k, 1)

    for k in (0, 1):
        send_w(g, k, 0, True)
    answers = number([flag for flag, _ in later])

    @pl.when(answers > 0)
    def _():
        pl.semaphore_wait(ready, answers)

    for k in (0, 1):
        send_w(g, k, 1, True)
    w_load.wait()
    for side in (0, 1):
        @pl.when(brief[side])
        def _():
            for k in (2, 3):
                send_w(g, k, side)


    @pl.when(end)
    def _():
        @pl.loop(2, n)
        def _(k):
            send_own(k)

    for load in loads:
        load.wait()

    def token_rows(pp, mm):
        s = pp * mp_size + mm
        return (pl.ds(pl.multiple_of(s * vr, vr), vr), pl.ds(pl.multiple_of(vlm_rows + s * ar, ar), ar))

    step = 32

    @pl.loop(0, vr // step)
    def _(i):
        o = pl.multiple_of(i * step, step)
        tok[pl.ds(pl.multiple_of((p * mp_size + m) * vr + o, step), step), :] = normalize(
            vlm_ref[pl.ds(o, step), :], gain_ref[...])

    @pl.loop(0, ar // step)
    def _(i):
        o = pl.multiple_of(i * step, step)
        tok[pl.ds(pl.multiple_of(vlm_rows + (p * mp_size + m) * ar + o, step), step), :] = normalize(
            act_ref[pl.ds(o, step), :], gain_ref[...])

    def tok_copy(pp, mm, part, to, slot):
        rows = token_rows(pp, mm)[part]
        return pltpu.make_async_remote_copy(
            src_ref=tok.at[rows, :], dst_ref=tok.at[rows, :], send_sem=tok_send,
            recv_sem=tok_recv.at[slot, 0 if slot == 3 else part], device_id=to, device_id_type=MESH)

    m_y = (1 - y) * 2 + c
    for part in (1, 0):
        tok_copy(p, m, part, xpart, 0).start()
        tok_copy(p, m, part, ypart, 1).start()
    for part in (1, 0):
        tok_copy(p, m, part, sibling, 3).start()

    def far_token_copy(part, c_from):
        rows = token_rows(p, m)[part]
        at = pl.ds(pl.multiple_of(c_from * ar + 2 * vr if part else c_from * vr, math.gcd(vr, ar)), (vr, ar)[part])
        return pltpu.make_async_remote_copy(
            src_ref=tok.at[rows, :], dst_ref=far_tok.at[at, :], send_sem=ft_send, recv_sem=ft_recv,
            device_id=(inward * 2 + p, y * 2 + 1), device_id_type=MESH)

    if far:
        @pl.when(end)
        def _():
            for part in (0, 1):
                far_token_copy(part, c).start()

    def far_w_copy(panel, to, slot):
        at = far_w.at[:, pl.ds(pl.multiple_of(panel * width, width), width)]
        return pltpu.make_async_remote_copy(
            src_ref=at if slot == 3 else wbuf.at[:, chunk(0)], dst_ref=at, send_sem=fw_send, recv_sem=fw_recv.at[slot],
            device_id=to, device_id_type=MESH)

    def spread_far_w():
        @pl.when(near & (c == 0))
        def _():
            far_w_copy(y * 2 + p, (g * 2 + 1 - p, y * 2 + 1), 1).start()
            far_w_copy(y * 2 + p, (d, (1 - y) * 2 + 1), 2).start()
            far_w_copy(y * 2 + p, sibling, 0).start()

    def relay_far_w():
        @pl.when(near & (c == 1))
        def _():
            far_w_copy(y * 2 + 1 - p, ypart, 1).wait_recv()
            far_w_copy(y * 2 + 1 - p, ypart, 3).start()

    def far_hid_copies(phase):
        for step_y in (0, 1):
            y_to = y if step_y == 0 else 1 - y
            for step_p in (0, 1):
                b = p if step_p == 0 else 1 - p
                cols_at = pl.ds(pl.multiple_of((y_to * 2 + b) * width, width), width)
                if 1 + step_y == phase:
                    yield pltpu.make_async_remote_copy(
                        src_ref=far_hid.at[pl.ds(2 * vr, 2 * ar), cols_at],
                        dst_ref=act_out.at[pl.ds(pl.multiple_of(y * 2 * ar, 2 * ar), 2 * ar), out_cols(b, chunk(0))],
                        send_sem=fh_send, recv_sem=fh_recv, device_id=(toward * 2 + p, y_to * 2), device_id_type=MESH)
                if (0 if step_p else 1 + step_y) == phase:
                    yield pltpu.make_async_remote_copy(
                        src_ref=far_hid.at[pl.ds(0, 2 * vr), cols_at],
                        dst_ref=vlm_out.at[pl.ds(pl.multiple_of((p * mp_size + y * 2) * vr, 2 * vr), 2 * vr), chunk(0)],
                        send_sem=fh_send, recv_sem=fh_recv, device_id=(toward * 2 + b, y_to * 2), device_id_type=MESH)

    def far_compute():
        @pl.when(near & (c == 1))
        def _():
            pltpu.make_async_remote_copy(
                src_ref=far_tok, dst_ref=far_tok, send_sem=ft_send, recv_sem=ft_recv,
                device_id=sibling, device_id_type=MESH).wait_recv()
            far_w_copy(y * 2, sibling, 0).wait_recv()
            far_w_copy(y * 2, sibling, 2).wait_recv()
            far_w_copy(y * 2, sibling, 3).wait_recv()

            @pl.loop(0, 2)
            def _(i):
                rows = pl.ds(pl.multiple_of(i * (vr + ar), math.gcd(vr, ar)), vr + ar)

                @pl.loop(0, 2)
                def _(j):
                    at = pl.ds(pl.multiple_of(j * 2 * width, width), 2 * width)
                    pre = jnp.dot(far_tok[rows, :], far_w[:, at], preferred_element_type=jnp.float32)
                    far_hid[rows, at] = gelu(pre)

            for copy in far_hid_copies(0):
                copy.start()

    def relay_first():
        tok_copy(1 - p, m, 1, sibling, 0).wait_recv()
        tok_copy(1 - p, m, 1, ypart, 2).start()
        tok_copy(p, m_y, 1, sibling, 1).wait_recv()
        tok_copy(p, m_y, 0, sibling, 1).wait_recv()
        tok_copy(p, m_y, 0, xpart, 2).start()
        tok_copy(1 - p, m, 0, sibling, 0).wait_recv()
        for part in (1, 0):
            tok_copy(1 - p, m, part, sibling, 3).start()
            tok_copy(p, m_y, part, sibling, 3).start()

    def relay_second():
        for part in (0, 1):
            tok_copy(1 - p, m_y, part, sibling, 2).wait_recv()
            tok_copy(1 - p, m_y, part, sibling, 3).start()

    def all_tokens():
        count = mp_size * (vr + ar)
        there = tok.at[pl.ds(0, count), :]
        pltpu.make_async_remote_copy(
            src_ref=there, dst_ref=there, send_sem=tok_send, recv_sem=tok_recv.at[3, 0],
            device_id=sibling, device_id_type=MESH).wait_recv()

    ex = pltpu.make_async_remote_copy(
        src_ref=wbuf.at[pl.ds(pl.multiple_of(g * r + (1 - p) * half, half), half), :],
        dst_ref=new_out.at[:, pl.ds(pl.multiple_of(p * cols, cols), cols)],
        send_sem=ex_send, recv_sem=ex_recv, device_id=xpart, device_id_type=MESH)
    kept = pltpu.make_async_copy(
        wbuf.at[pl.ds(pl.multiple_of(g * r + p * half, half), half), :],
        new_out.at[:, pl.ds(pl.multiple_of(p * cols, cols), cols)], loc_sem.at[0])

    def arrive_at(t, i):
        k = t - i
        inside = (k >= 0) & (k < n) & jnp.logical_not(short & (k == 0))

        @pl.when(inside & (g - 1 - i >= 0))
        def _():
            w_arrival(g - 1 - i, k).wait_recv()
            send_w(g - 1 - i, k, 1)

        @pl.when(inside & (g + 1 + i < groups))
        def _():
            w_arrival(g + 1 + i, k).wait_recv()
            send_w(g + 1 + i, k, 0)

    def send_next(t):
        for side in (0, 1):
            ahead = jnp.where(brief[side] & (t < 2), 4, jnp.where(last[side] & (t >= 2), 1, 2))
            k = jnp.where(last[side] & (t == n - 1), t, t + ahead)
            pause = last[side] & ((t == 2) | (t == n - 2)) | brief[side] & (t >= 2) & (t < n - 3)

            @pl.when((k < n) & jnp.logical_not(end) & jnp.logical_not(pause))
            def _():
                send_w(g, k, side)

    def arrive_far(t):
        arrive_at(t, groups - 2)

    def arrive_near(t):
        @pl.loop(0, groups - 3)
        def _(i):
            arrive_at(t, groups - 3 - i)

        held = end & far & (t >= n - 1)

        @pl.when(jnp.logical_not(held))
        def _():
            arrive_at(t, 0)

        if t == n:
            @pl.when(held)
            def _():
                arrive_at(n - 1, 0)

        send_next(t)

    def arrive(t):
        @pl.loop(0, groups - 1)
        def _(i):
            arrive_at(t, i)

        send_next(t)

    tile = math.gcd(256, math.gcd(vlm_rows, act_rows))
    a_tiles, v_tiles = act_rows // tile, vlm_rows // tile

    def out_cols(side, cc):
        return pl.ds(pl.multiple_of(side * cols + cc.start, width), cc.size)

    def tile_rows(start):
        return pl.ds(pl.multiple_of(start, tile), tile)

    def hid_copy(cc, t):
        return pltpu.make_async_remote_copy(
            src_ref=hid.at[tile_rows(vlm_rows + (1 - p) * act_rows + t * tile), cc],
            dst_ref=act_out.at[tile_rows(t * tile), out_cols(p, cc)],
            send_sem=hid_send, recv_sem=hid_recv, device_id=xpart, device_id_type=MESH)

    def own_copy(cc):
        return pltpu.make_async_copy(
            hid.at[pl.ds(pl.multiple_of(vlm_rows + p * act_rows, act_rows), act_rows), cc],
            act_out.at[:, out_cols(p, cc)], loc_sem.at[1])

    def vlm_copy(cc):
        return pltpu.make_async_copy(hid.at[pl.ds(0, vlm_rows), cc], vlm_out.at[:, cc], loc_sem.at[2])

    def hidden(rows, cc):
        pre = jnp.dot(tok[rows, :], wbuf[:, cc], preferred_element_type=jnp.float32)
        hid[rows, cc] = gelu(pre)

    def for_partner(cc):
        @pl.loop(0, a_tiles)
        def _(t):
            hidden(tile_rows(vlm_rows + (1 - p) * act_rows + t * tile), cc)
            hid_copy(cc, t).start()

    def for_self(cc):
        @pl.loop(0, a_tiles + v_tiles)
        def _(t):
            hidden(tile_rows(jnp.where(
                t < a_tiles, vlm_rows + p * act_rows + t * tile, (t - a_tiles) * tile)), cc)

    warm = groups - 1

    @pl.loop(0, warm)
    def _(t):
        arrive(t)

    relay_first()
    if far:
        spread_far_w()

    @pl.when(jnp.logical_not(near))
    def _():
        ex.start()

    kept.start()
    arrive(warm)
    arrive(warm + 1)
    relay_second()
    arrive(warm + 2)
    if far:
        relay_far_w()

    @pl.when(near)
    def _():
        ex.start()

    all_tokens()

    def pair_at(j, body):
        if far and j == 0:
            @pl.when(short)
            def _():
                body(chunk(1))

            @pl.when(jnp.logical_not(short))
            def _():
                body(chunk(0, 2))
        else:
            body(chunk(j, 2))

    for j in range(0, 4, 2):
        pair_at(j, for_partner)
    for j in range(0, 4, 2):
        pair_at(j, for_self)
    for j in range(4, n):
        arrive_far(warm + j - 1)
        if far and j == n - 2:
            far_compute()
        if far and j == n - 1:
            @pl.when(near & (c == 1))
            def _():
                for copy in far_hid_copies(1):
                    copy.start()

        for_partner(chunk(j))
        arrive_near(warm + j - 1)
        if j % 2 == 1:
            for_self(chunk(j - 1, 2))

    tail_cols, all_cols = chunk(1, n - 1), chunk(0, n)

    def by_width(brief, body):
        @pl.when(brief)
        def _():
            body(tail_cols)

        @pl.when(jnp.logical_not(brief))
        def _():
            body(all_cols)

    def copy_out(cc):
        own_copy(cc).start()
        vlm_copy(cc).start()

    def copied_out(cc):
        own_copy(cc).wait()
        vlm_copy(cc).wait()

    by_width(short, copy_out)

    def w_sent(block, side):
        for skip in (0, 1):
            for fewer in (0, late):
                few = w_last(block, side)

                @pl.when((brief[side] if skip else jnp.logical_not(brief[side])) & (few if fewer else jnp.logical_not(few)))
                def _():
                    w_copy(block, chunk(0, n - skip - fewer), w_slot(block, side), ex_recv, side).wait_send()

    if far:
        @pl.when(near & (c == 1))
        def _():
            for side in (0, 1):
                @pl.when(last[side])
                def _():
                    w_sent(groups - 1 if side == 0 else 0, side)

            for copy in far_hid_copies(2):
                copy.start()

    @pl.loop(0, groups)
    def _(block):
        @pl.when(has_left & (block >= g) & jnp.logical_not(w_last(block, 0) & (c == 1)))
        def _():
            w_sent(block, 0)

        @pl.when(has_right & (block <= g) & jnp.logical_not(w_last(block, 1) & (c == 1)))
        def _():
            w_sent(block, 1)

    def bytes_of(ref, send, recv):
        return pltpu.make_async_remote_copy(
            src_ref=ref, dst_ref=ref, send_sem=send, recv_sem=recv, device_id=sibling, device_id_type=MESH)

    if far:
        @pl.when(near & (c == 1))
        def _():
            bytes_of(far_w.at[:, pl.ds(0, width)], fw_send, ex_recv).wait_send()
            bytes_of(hid.at[pl.ds(0, 8 * (vr + ar)), chunk(0)], fh_send, ex_recv).wait_send()

        @pl.when(near & (c == 0))
        def _():
            bytes_of(wbuf.at[:, pl.ds(0, 3 * width)], fw_send, ex_recv).wait_send()

        @pl.when(near)
        def _():
            bytes_of(wbuf.at[pl.ds(0, r), chunk(0, late)], w_send.at[groups + 1], ex_recv).wait_send()

        @pl.when(end)
        def _():
            bytes_of(tok.at[pl.ds(0, vr + ar), :], ft_send, ex_recv).wait_send()

    bytes_of(tok.at[pl.ds(0, 7 * (vr + ar)), :], tok_send, ex_recv).wait_send()
    ex.wait_send()
    taken = new_out.at[:, pl.ds(pl.multiple_of((1 - p) * cols, cols), cols)]
    bytes_of(taken, ex_send, ex_recv).wait_recv()
    kept.wait()

    def exchanged(cc):
        there = act_out.at[:, out_cols(1 - p, cc)]
        bytes_of(there, hid_send, hid_recv).wait_send()
        bytes_of(there, hid_send, hid_recv).wait_recv()

    by_width(short, copied_out)
    by_width(short, exchanged)
    if far:
        @pl.when(short)
        def _():
            bytes_of(hid.at[:, chunk(0)], fh_send, fh_recv).wait_recv()


def store(*refs):
    count = (len(refs) - 1) // 2
    copies = [pltpu.make_async_copy(refs[i], refs[count + i], refs[-1].at[i]) for i in range(count)]
    for copy in copies:
        copy.start()
    for copy in copies:
        copy.wait()


def solution(mesh):
    groups, mp_size = mesh.shape["dp"] // 2, mesh.shape["mp"]

    def local(vlm_tokens, action_tokens, norm_gain, proj_old):
        vr, ar = vlm_tokens.shape[0], action_tokens.shape[0]
        features = vlm_tokens.shape[1]
        r, cols = proj_old.shape
        vlm_rows, act_rows = 2 * mp_size * vr, mp_size * ar
        bf16 = jnp.bfloat16
        dma = pltpu.SemaphoreType.DMA
        hbm, anywhere = pl.BlockSpec(memory_space=pltpu.HBM), pl.BlockSpec(memory_space=pl.ANY)
        chunks = cols // chunk_width(cols)
        shapes = (
            jax.ShapeDtypeStruct((vlm_rows, cols), bf16),
            jax.ShapeDtypeStruct((act_rows, 2 * cols), bf16),
            jax.ShapeDtypeStruct((r // 2, 2 * cols), bf16),
        )
        results = pl.pallas_call(
            functools.partial(kernel, groups, mp_size),
            name="up_gelu",
            out_shape=shapes,
            in_specs=[hbm] * 4,
            out_specs=(anywhere,) * 3,
            scratch_shapes=[
                pltpu.VMEM((vr, features), bf16),
                pltpu.VMEM((ar, features), bf16),
                pltpu.VMEM((1, features), jnp.float32),
                pltpu.VMEM((vlm_rows + 2 * act_rows, features), bf16),
                pltpu.VMEM((groups * r, cols), bf16),
                pltpu.VMEM((vlm_rows + 2 * act_rows, cols), bf16),
                dma, dma((4, 2)), dma((groups + 2,)), dma((groups - 1, chunks)), dma, dma, dma, dma, dma((4,)), dma((3,)),
                pltpu.VMEM((2 * (vr + ar), features), bf16),
                pltpu.VMEM((groups * r, 4 * chunk_width(cols)), bf16),
                pltpu.VMEM((2 * (vr + ar), 4 * chunk_width(cols)), bf16),
                dma, dma, dma, dma((4,)), dma, dma, pltpu.SemaphoreType.REGULAR,
            ],
            compiler_params=pltpu.CompilerParams(
                collective_id=0, has_side_effects=True, vmem_limit_bytes=48 * 1024 * 1024),
        )(*[pltpu.with_memory_space_constraint(array, pltpu.HBM) for array in (
            vlm_tokens, action_tokens, norm_gain.reshape(1, -1), proj_old)])
        return pl.pallas_call(
            store,
            name="store",
            out_shape=shapes,
            in_specs=[anywhere] * 3,
            out_specs=(hbm,) * 3,
            scratch_shapes=[dma((3,))],
            compiler_params=pltpu.CompilerParams(vmem_limit_bytes=1024 * 1024),
        )(*results)

    return jax.shard_map(
        local,
        mesh=mesh,
        in_specs=(P(("dp", "mp"), None), P(("dp", "mp"), None), P(), P("dp", "mp")),
        out_specs=(P("dp", "mp"), P("dp", "mp"), P("dp", "mp")),
        check_vma=False,
    )
```
